512 devices in a mesh: row: 32 (over y, x), col: 16 (over z, core).
Axes of the slice: x: 4, y: 8, z: 8, core: 2. Of those that a mesh axis runs over, the one named last changes fastest.
Arguments:
- tokens: bfloat16 [24576, 2048], P('row', 'col'), may hold values from -6 to 6
- out_grad: bfloat16 [24576, 2048], P('row', 'col'), may hold values from -3072 to 3072
- counts: int32 [32], P('row'), may hold values from 65 to 768
- block_moves: int32 [16, 3], replicated, may hold values from 0 to 31, as said below
- segment_ids: int32 [24576], P('row'), may hold values from 0 to 767, never falling along the last dimension, each value on 1 to 128 neighbouring positions
- gate_weight: bfloat16 [2048, 8192], P('row', 'col'), may hold values from -0.125 to 0.125
- up_weight: bfloat16 [2048, 8192], P('row', 'col'), may hold values from -0.125 to 0.125
- down_weight: bfloat16 [2048, 8192], P('row', 'col'), may hold values from -0.0625 to 0.0625
Outputs:
- hidden: bfloat16 [16384, 8192], P('row', 'col')
- gate_grad: float32 [2048, 8192], P('row', 'col')
- up_grad: float32 [2048, 8192], P('row', 'col')
- down_grad: float32 [2048, 8192], P('row', 'col')
The draws below stay inside these ranges and needn't reach their ends.
Inputs may be any that keep to these rules, and one draw needn't show every extreme that they name: `block_moves`: each row is (source rank, destination rank, block index); the block is a valid block of its source; no two rows share both source and destination, nor both source and block; a rank is the source of at most two rows or the destination of at most one, never both; after the moves every rank holds at most 4 valid blocks and some hold exactly 4. `segment_ids`: never falling along the whole array; each document covers 1 to 128 consecutive slots.
All inputs are finite; a program needn't handle non-finite values.
Results may differ from the reference program's by a relative error of at most 0.015.
Values may be sent and summed in bfloat16 or wider, within the bound.
No kernel may reach another device: no remote copies, remote signals or barrier semaphores. Data moves between devices by JAX's collectives and lax.ppermute only.
A program may use at most 64 MiB of HBM per device.

```python
import math
import jax
import jax.numpy as jnp
import numpy as np
from jax import lax

D = 2048
F = 8192
BLOCK = 128
WORK = 4
CAP = 6
TOK_DEV = 768
TOKENS = 24576
MOVES = 16
N_ROW = 32


def rebalance_plan(key):
    perm_key, light_key, part_key, pick_key, flip_key = jax.random.split(key, 5)
    groups = N_ROW // 4
    half = N_ROW // 2
    pair_order = jax.random.permutation(perm_key, half).astype(jnp.int32).reshape(groups, 2)
    flips = jax.random.randint(flip_key, (groups, 2), 0, 2, dtype=jnp.int32)
    low_rank = pair_order
    high_rank = pair_order + half
    first_rank = jnp.where(flips == 0, low_rank, high_rank)
    second_rank = jnp.where(flips == 0, high_rank, low_rank)
    order_ranks = jnp.stack([first_rank[:, 0], second_rank[:, 0], first_rank[:, 1], second_rank[:, 1]], axis=1).astype(jnp.int32)
    spare_load = jax.random.randint(light_key, (groups,), 1, WORK + 1, dtype=jnp.int32)
    heavy_load = jnp.full((groups,), WORK + 2, jnp.int32)
    lean_load = jnp.full((groups,), WORK - 1, jnp.int32)
    all_loads = jnp.stack([heavy_load, lean_load, lean_load, spare_load], axis=1).reshape(-1)
    block_counts = jnp.zeros((N_ROW,), jnp.int32).at[order_ranks.reshape(-1)].set(all_loads)
    tail_fill = jax.random.randint(part_key, (N_ROW,), BLOCK // 2 + 1, BLOCK + 1, dtype=jnp.int32)
    counts = ((block_counts - 1) * BLOCK + tail_fill).astype(jnp.int32)
    chosen = jax.vmap(lambda sub_key: jax.random.permutation(sub_key, WORK + 2)[:2])(jax.random.split(pick_key, groups)).astype(jnp.int32)
    first_move = jnp.stack([order_ranks[:, 0], order_ranks[:, 1], chosen[:, 0]], axis=1)
    second_move = jnp.stack([order_ranks[:, 0], order_ranks[:, 2], chosen[:, 1]], axis=1)
    block_moves = jnp.stack([first_move, second_move], axis=1).reshape(N_ROW // 2, 3).astype(jnp.int32)
    return (counts, block_moves)


def draw_counts(key, part):
    return rebalance_plan(jax.random.fold_in(key, 11))[0]


def draw_block_moves(key, part):
    return rebalance_plan(jax.random.fold_in(key, 11))[1]


def level_of(key, extent, cuts, smallest, largest):
    loudness, own = 1.0, jax.random.fold_in(key, 6)
    for dim, shards_of in cuts:
        steps = jnp.exp(jax.random.uniform(jax.random.fold_in(own, dim), (shards_of,), jnp.float32, smallest / len(cuts), largest / len(cuts)))
        loudness = loudness * jnp.repeat(steps, extent[dim] // shards_of).reshape([-1 if axis == dim else 1 for axis in range(len(extent))])
    return loudness


def length_profile(number_of, total, reach, slope):
    loads = [(1 << 20) // math.isqrt(rank ** slope) + 1 for rank in range(2, number_of + 1)]
    surplus, given = total - reach - (number_of - 1), [1] * (number_of - 1)
    while surplus > 0:
        candidates = [i for i in range(number_of - 1) if given[i] < reach]
        mass, left = sum([loads[i] for i in candidates]), surplus
        for i in candidates:
            extra = min(reach - given[i], max(1, left * loads[i] // mass), surplus)
            given[i] = given[i] + extra
            surplus = surplus - extra
    return np.array([reach] + given)


def uneven_parts(rng, number_of, total, most, lean):
    if number_of == 2:
        one = jax.random.randint(rng, (), max(1, total - most), min(most, total - 1) + 1)
        return jnp.stack([one, total - one])
    sizes = jnp.asarray(length_profile(number_of, total, most, lean), jnp.int32)
    twos = (number_of - 1) // 2
    source_of, sink = sizes[1:1 + 2 * twos:2], sizes[2:2 + 2 * twos:2]
    slack = jnp.minimum(source_of - 1, most - sink)
    passed = jax.random.randint(jax.random.fold_in(rng, 1), (twos,), 0, 1 << 20) % (slack + 1)
    sizes = sizes.at[1:1 + 2 * twos:2].set(source_of - passed).at[2:2 + 2 * twos:2].set(sink + passed)
    return sizes[jax.random.permutation(jax.random.fold_in(rng, 2), number_of)]


def scatter_about(rng, extent, spread, limit, cuts=(), held_as=jnp.bfloat16):
    result = jax.random.normal(rng, extent, jnp.float32) * spread
    if len(cuts) > 0:
        result = level_of(rng, extent, cuts, -0.22, 0.18) * result
    return jnp.clip(result, min=-limit, max=limit).astype(held_as)


def setup_inputs(seed: int = 0) -> dict:
    splits = jax.random.split(jax.random.key(seed), 9)
    return {
        "tokens": scatter_about(splits[0], (TOKENS, D), 1.0, 6.0, ((0, 32), (1, 16))),
        "out_grad": scatter_about(splits[1], (TOKENS, D), (16 * N_ROW), 3072.0, ((0, 32), (1, 16))),
        "counts": draw_counts(jax.random.fold_in(splits[8], 71), 0),
        "block_moves": draw_block_moves(jax.random.fold_in(splits[8], 71), 0),
        "segment_ids": jnp.searchsorted(jnp.cumsum(uneven_parts(splits[4], TOKENS // 32, TOKENS, 128, 2)), jnp.arange(TOKENS), side="right").astype(jnp.int32),
        "gate_weight": scatter_about(splits[5], (D, F), D ** -0.5, 0.125, ((0, 32), (1, 16))),
        "up_weight": scatter_about(splits[6], (D, F), D ** -0.5, 0.125, ((0, 32), (1, 16))),
        "down_weight": scatter_about(splits[7], (D, F), F ** -0.5, 0.0625, ((0, 32), (1, 16))),
    }


def loss_mask(counts, segment_ids):
    segments = segment_ids.reshape(N_ROW, TOK_DEV)
    following = jnp.concatenate([segments[:, 1:], segments[:, -1:]], axis=1)
    places = jnp.arange(TOK_DEV, dtype=jnp.int32)[None, :]
    kept_flag = (places + 1 < counts[:, None]) & (following == segments)
    return kept_flag.astype(jnp.float32)


def work_index(counts, block_moves):
    source = block_moves[:, 0]
    target = block_moves[:, 1]
    block_id = block_moves[:, 2]
    rank_ids = jnp.arange(N_ROW, dtype=jnp.int32)
    block_ids = jnp.arange(CAP, dtype=jnp.int32)
    filled = (counts + BLOCK - 1) // BLOCK
    moved_out = jnp.any((source[None, None, :] == rank_ids[:, None, None]) & (block_id[None, None, :] == block_ids[None, :, None]), axis=2)
    kept_flag = (block_ids[None, :] < filled[:, None]) & jnp.logical_not(moved_out)
    arrive = target[None, :] == rank_ids[:, None]
    flag_bits = jnp.concatenate([kept_flag, arrive], axis=1).astype(jnp.int32)
    own_ids = (rank_ids[:, None] * CAP + block_ids[None, :]).astype(jnp.int32)
    came_ids = jnp.broadcast_to((source * CAP + block_id)[None, :], (N_ROW, MOVES)).astype(jnp.int32)
    source_ids = jnp.concatenate([own_ids, came_ids], axis=1)
    list_place = (jnp.cumsum(flag_bits, axis=1) - 1).astype(jnp.int32)
    slot_ids = jnp.arange(WORK, dtype=jnp.int32)
    slot_hit = (flag_bits[:, :, None] == 1) & (list_place[:, :, None] == slot_ids[None, None, :])
    chosen = jnp.sum(jnp.where(slot_hit, source_ids[:, :, None] + 1, 0), axis=1).astype(jnp.int32)
    return (chosen - 1).astype(jnp.int32)


def pick_blocks(block_rows, slot_index):
    flat_index = slot_index.reshape(-1)
    picked = jnp.take(block_rows, jnp.maximum(flat_index, 0), axis=0)
    live_rows = (flat_index >= 0).reshape((-1,) + (1,) * (picked.ndim - 1))
    return jnp.where(live_rows, picked, jnp.zeros_like(picked))


def local_terms(gate_sum, up_sum, back_sum):
    logistic = jax.nn.sigmoid(gate_sum)
    activated = gate_sum * logistic
    hidden = (activated * up_sum).astype(jnp.bfloat16)
    gate_back = (back_sum * up_sum * logistic * (1.0 + gate_sum * (1.0 - logistic))).astype(jnp.bfloat16)
    up_back = (back_sum * activated).astype(jnp.bfloat16)
    return hidden, gate_back, up_back


def contract(left_side, right_side):
    return lax.dot_general(left_side, right_side, (((0,), (0,)), ((), ())), preferred_element_type=jnp.float32)


def reference(tokens, out_grad, counts, block_moves, segment_ids, gate_weight, up_weight, down_weight):
    weight_mask = loss_mask(counts, segment_ids)
    loss_total = jnp.sum(weight_mask)
    slot_index = work_index(counts, block_moves)
    work_tokens = pick_blocks(tokens.reshape(N_ROW * CAP, BLOCK, D), slot_index).reshape(N_ROW, WORK * BLOCK, D)
    work_grad = pick_blocks(out_grad.reshape(N_ROW * CAP, BLOCK, D), slot_index).reshape(N_ROW, WORK * BLOCK, D)
    work_weight = pick_blocks(weight_mask.reshape(N_ROW * CAP, BLOCK), slot_index).reshape(N_ROW, WORK * BLOCK)

    def per_rank(running, inputs):
        tok_rows, grad_rows, row_weight = inputs
        gate_sum = jnp.dot(tok_rows, gate_weight, preferred_element_type=jnp.float32)
        up_sum = jnp.dot(tok_rows, up_weight, preferred_element_type=jnp.float32)
        back_sum = jnp.dot(grad_rows, down_weight, preferred_element_type=jnp.float32) * row_weight[:, None]
        hidden, gate_back, up_back = local_terms(gate_sum, up_sum, back_sum)
        weighted = grad_rows * row_weight.astype(jnp.bfloat16)[:, None]
        new_terms = (contract(tok_rows, gate_back), contract(tok_rows, up_back), contract(weighted, hidden))
        rounded = tuple(lax.optimization_barrier((term_sum / loss_total).astype(jnp.bfloat16)).astype(jnp.float32) for term_sum in new_terms)
        return tuple(total_part + new_part for total_part, new_part in zip(running, rounded)), hidden

    zero_sums = jnp.zeros((D, F), jnp.float32)
    grad_sums, hidden_all = lax.scan(per_rank, (zero_sums, zero_sums, zero_sums), (work_tokens, work_grad, work_weight))
    return hidden_all.reshape(N_ROW * WORK * BLOCK, F), grad_sums[0], grad_sums[1], grad_sums[2]
```

```python
import jax
import jax.numpy as jnp
from jax import lax
from jax.experimental import pallas as pl
from jax.experimental.pallas import tpu as pltpu
from jax.sharding import Mesh
from jax.sharding import PartitionSpec as P

BLOCK = 128
WORK = 4
CAP = 6
NY, NX, NZ = 8, 4, 8
ROW = ("y", "x")
COL = ("z", "c")
NTAG = 16
SIDE = 768


def vmem():
    return pl.BlockSpec(memory_space=pltpu.VMEM)


def smem():
    return pl.BlockSpec(memory_space=pltpu.SMEM)


def params(**kw):
    return pltpu.CompilerParams(vmem_limit_bytes=60 * 1024 * 1024, **kw)


def move_count(moves):
    return moves.shape[0] // 3


def pack_x(pos, moves, mask, tok, grad, box, masked):
    me = pos[0] * NX + pos[1]
    for b in range(CAP):
        rows = slice(b * BLOCK, (b + 1) * BLOCK)
        wide = jnp.broadcast_to(mask[b : b + 1, :], (BLOCK, BLOCK)).T
        masked[rows, :] = (grad[rows, :].astype(jnp.float32) * wide).astype(jnp.bfloat16)
    tally = jnp.sum(mask[...], axis=0, keepdims=True)
    for d in range(NX):
        box[d, 4 * BLOCK :, :] = jnp.broadcast_to(tally, (NTAG, BLOCK)).astype(jnp.bfloat16)

    def body(m, seen):
        src, dst, blk = moves[3 * m], moves[3 * m + 1], moves[3 * m + 2]
        mine = src == me

        @pl.when(mine)
        def _():
            peer = dst % NX
            at = pl.multiple_of(seen * (2 * BLOCK), BLOCK)
            start = pl.multiple_of(blk * BLOCK, BLOCK)
            box[peer, pl.ds(at, BLOCK), :] = tok[pl.ds(start, BLOCK), :]
            box[peer, pl.ds(at + BLOCK, BLOCK), :] = masked[pl.ds(start, BLOCK), :]

        return jnp.where(mine, jnp.minimum(seen + 1, 1), seen)

    lax.fori_loop(0, move_count(moves), body, 0)


def pack_y(pos, moves, got, box, seen):
    my, mx = pos[0], pos[1]
    for i in range(NX):
        seen[i] = 0
    tally = got[0, 4 * BLOCK :, :].astype(jnp.float32)
    for i in range(1, NX):
        tally = tally + got[i, 4 * BLOCK :, :].astype(jnp.float32)
    for d in range(NY):
        box[d, 2 * BLOCK :, :] = tally.astype(jnp.bfloat16)

    def body(m, carry):
        src, dst = moves[3 * m], moves[3 * m + 1]

        @pl.when(src // NX == my)
        def _():
            sx = src % NX
            nth = seen[sx]
            seen[sx] = jnp.minimum(nth + 1, 1)

            @pl.when(dst % NX == mx)
            def _():
                at = pl.multiple_of(nth * (2 * BLOCK), BLOCK)
                box[dst // NX, : 2 * BLOCK, :] = got[sx, pl.ds(at, 2 * BLOCK), :]

        return carry

    lax.fori_loop(0, move_count(moves), body, 0)


def fill_work(pos, moves, tok, masked, got, box, total):
    me = pos[0] * NX + pos[1]
    count = pos[2]
    span = WORK * BLOCK
    tally = got[0, 2 * BLOCK : 2 * BLOCK + 8, :].astype(jnp.float32)
    for i in range(1, NY):
        tally = tally + got[i, 2 * BLOCK : 2 * BLOCK + 8, :].astype(jnp.float32)
    total[...] = jnp.broadcast_to(jnp.sum(tally, axis=1, keepdims=True), total.shape)
    box[0] = jnp.zeros_like(box[0])

    def put(slot, t, g):
        at = pl.multiple_of(slot * BLOCK, BLOCK)
        box[0, pl.ds(at, BLOCK), :] = t
        box[0, pl.ds(at + span, BLOCK), :] = g

    def own(b, nth):
        def gone(m, hit):
            return hit | ((moves[3 * m] == me) & (moves[3 * m + 2] == b)).astype(jnp.int32)

        left = lax.fori_loop(0, move_count(moves), gone, 0)
        keep = (b * BLOCK < count) & (left == 0)

        @pl.when(keep & (nth < WORK))
        def _():
            start = pl.multiple_of(b * BLOCK, BLOCK)
            put(nth, tok[pl.ds(start, BLOCK), :], masked[pl.ds(start, BLOCK), :])

        return nth + keep.astype(jnp.int32)

    nth = lax.fori_loop(0, CAP, own, 0)

    def came(m, nth):
        src, dst = moves[3 * m], moves[3 * m + 1]
        here = dst == me

        @pl.when(here & (nth < WORK))
        def _():
            sy = src // NX
            put(nth, got[sy, :BLOCK, :], got[sy, BLOCK : 2 * BLOCK, :])

        return nth + here.astype(jnp.int32)

    lax.fori_loop(0, move_count(moves), came, nth)
    for d in range(1, NZ):
        box[d] = box[0]


def forward(pos, mine, other, wg, wu, wd, hidden, gate_back, up_back, tok, grad):
    span = WORK * BLOCK

    @pl.when(pl.program_id(0) == 0)
    def _():
        first = pos[3] == 0
        for z in range(NZ):
            a, b = mine[z], other[z]
            low = jnp.where(first, a, b)
            high = jnp.where(first, b, a)
            at = z * 2 * BLOCK
            tok[:, at : at + BLOCK] = low[:span]
            grad[:, at : at + BLOCK] = low[span:]
            tok[:, at + BLOCK : at + 2 * BLOCK] = high[:span]
            grad[:, at + BLOCK : at + 2 * BLOCK] = high[span:]

    gate_sum = jnp.dot(tok[...], wg[...], preferred_element_type=jnp.float32)
    up_sum = jnp.dot(tok[...], wu[...], preferred_element_type=jnp.float32)
    back_sum = jnp.dot(grad[...], wd[...], preferred_element_type=jnp.float32)
    logistic = jax.nn.sigmoid(gate_sum)
    act = gate_sum * logistic
    hidden[...] = (act * up_sum).astype(jnp.bfloat16)
    gate_back[...] = (back_sum * up_sum * logistic * (1.0 + gate_sum * (1.0 - logistic))).astype(
        jnp.bfloat16
    )
    up_back[...] = (back_sum * act).astype(jnp.bfloat16)


def gradients(total, tok, grad, hidden, gate_back, up_back, by_x, by_y):
    inv = 1.0 / total[0, 0]

    def term(left, right):
        out = lax.dot_general(
            left, right, (((0,), (0,)), ((), ())), preferred_element_type=jnp.float32
        )
        return (out * inv).astype(jnp.bfloat16)

    half = 256
    t, g = tok[...], grad[...]
    gate = term(t, gate_back[...])
    up = term(t, up_back[...])
    down = term(g, hidden[...])
    for x in range(NX):
        rows = slice(64 * x, 64 * (x + 1))
        by_x[x, 0, :, :512] = gate[rows]
        by_x[x, 0, :, 512:] = up[rows, :half]
    by_y[0, :, :half] = up[:, half:]
    by_y[0, :, half:] = down


def add_x(got, out):
    acc = got[0].astype(jnp.float32)
    for i in range(1, NX):
        acc = acc + got[i].astype(jnp.float32)
    out[...] = acc.astype(jnp.bfloat16)


def finish(from_y, from_x, gate, up, down):
    acc = from_y[0].astype(jnp.float32)
    for i in range(1, NY):
        acc = acc + from_y[i].astype(jnp.float32)
    bcc = from_x[0].astype(jnp.float32)
    for i in range(1, NX):
        bcc = bcc + from_x[i].astype(jnp.float32)
    gate[...] = acc[:, :512]
    up[:, :256] = acc[:, 512:]
    up[:, 256:] = bcc[:, :256]
    down[...] = bcc[:, 256:]


def a2a(value, axis):
    return lax.all_to_all(value, axis, split_axis=0, concat_axis=0, tiled=True)


def on_device(
    tokens, out_grad, counts, block_moves, segment_ids, gate_weight, up_weight, down_weight
):
    bf = jnp.bfloat16
    f32 = jnp.float32
    slots = tokens.shape[0]
    feat = tokens.shape[1]
    hid = gate_weight.shape[1]
    span = WORK * BLOCK
    model = 2 * NZ * feat
    weights = lax.all_gather(
        jnp.concatenate([gate_weight, up_weight, down_weight], axis=1), ROW, axis=0, tiled=True
    )

    count = counts[0]
    pos = jnp.stack([lax.axis_index("y"), lax.axis_index("x"), count, lax.axis_index("c")])
    moves = block_moves.reshape(-1)
    places = jnp.arange(slots, dtype=jnp.int32)
    following = jnp.concatenate([segment_ids[1:], segment_ids[-1:]])
    mask = ((places + 1 < count) & (following == segment_ids)).astype(f32).reshape(CAP, BLOCK)

    box, masked = pl.pallas_call(
        pack_x,
        out_shape=(
            jax.ShapeDtypeStruct((NX, 4 * BLOCK + NTAG, feat), bf),
            jax.ShapeDtypeStruct((slots, feat), bf),
        ),
        in_specs=[smem(), smem(), vmem(), vmem(), vmem()],
        out_specs=(vmem(), vmem()),
        compiler_params=params(),
        name="pack_x",
    )(pos, moves, mask, tokens, out_grad)
    got = a2a(box, "x")
    box = pl.pallas_call(
        pack_y,
        out_shape=jax.ShapeDtypeStruct((NY, 2 * BLOCK + NTAG, feat), bf),
        in_specs=[smem(), smem(), vmem()],
        out_specs=vmem(),
        scratch_shapes=[pltpu.SMEM((NX,), jnp.int32)],
        compiler_params=params(),
        name="pack_y",
    )(pos, moves, got)
    got = a2a(box, "y")
    box, total = pl.pallas_call(
        fill_work,
        out_shape=(
            jax.ShapeDtypeStruct((NZ, 2 * span, feat), bf),
            jax.ShapeDtypeStruct((8, BLOCK), f32),
        ),
        in_specs=[smem(), smem(), vmem(), vmem(), vmem()],
        out_specs=(vmem(), vmem()),
        compiler_params=params(),
        name="fill_work",
    )(pos, moves, tokens, masked, got)
    mine = a2a(box, "z")
    other = lax.ppermute(mine, "c", [(0, 1), (1, 0)])

    tile = 256
    steps = hid // tile

    def whole(shape):
        return pl.BlockSpec(shape, lambda j: (0,) * len(shape))

    def cols(rows, offset):
        return pl.BlockSpec((rows, tile), lambda j: (0, j + offset))

    hidden, gate_back, up_back, tok, grad = pl.pallas_call(
        forward,
        grid=(steps,),
        out_shape=(
            jax.ShapeDtypeStruct((span, hid), bf),
            jax.ShapeDtypeStruct((span, hid), bf),
            jax.ShapeDtypeStruct((span, hid), bf),
            jax.ShapeDtypeStruct((span, model), bf),
            jax.ShapeDtypeStruct((span, model), bf),
        ),
        in_specs=[
            smem(),
            whole((NZ, 2 * span, feat)),
            whole((NZ, 2 * span, feat)),
            cols(model, 0),
            cols(model, steps),
            cols(model, 2 * steps),
        ],
        out_specs=(
            cols(span, 0),
            cols(span, 0),
            cols(span, 0),
            whole((span, model)),
            whole((span, model)),
        ),
        compiler_params=params(dimension_semantics=("arbitrary",)),
        name="forward",
    )(pos, mine, other, weights, weights, weights)

    per = 64
    by_x, by_y = pl.pallas_call(
        gradients,
        grid=(NY,),
        out_shape=(
            jax.ShapeDtypeStruct((NX, NY, per, SIDE), bf),
            jax.ShapeDtypeStruct((NY, NX * per, SIDE), bf),
        ),
        in_specs=[
            pl.BlockSpec((8, BLOCK), lambda j: (0, 0)),
            pl.BlockSpec((span, NX * per), lambda j: (0, j)),
            pl.BlockSpec((span, NX * per), lambda j: (0, j)),
            whole((span, hid)),
            whole((span, hid)),
            whole((span, hid)),
        ],
        out_specs=(
            pl.BlockSpec((NX, 1, per, SIDE), lambda j: (0, j, 0, 0)),
            pl.BlockSpec((1, NX * per, SIDE), lambda j: (j, 0, 0)),
        ),
        compiler_params=params(dimension_semantics=("arbitrary",)),
        name="gradients",
    )(total, tok, grad, hidden, gate_back, up_back)

    part_y = lax.psum_scatter(
        by_y.reshape(NY * NX * per, SIDE), "y", scatter_dimension=0, tiled=True
    )
    part_x = pl.pallas_call(
        add_x,
        out_shape=jax.ShapeDtypeStruct((NY, per, SIDE), bf),
        in_specs=[vmem()],
        out_specs=vmem(),
        compiler_params=params(),
        name="add_x",
    )(a2a(by_x, "x"))
    from_y = a2a(part_x, "y")
    from_x = a2a(part_y.reshape(NX, per, SIDE), "x")
    gate_grad, up_grad, down_grad = pl.pallas_call(
        finish,
        out_shape=tuple(jax.ShapeDtypeStruct((per, hid), f32) for _ in range(3)),
        in_specs=[vmem(), vmem()],
        out_specs=(vmem(), vmem(), vmem()),
        compiler_params=params(),
        name="finish",
    )(from_y, from_x)
    return (hidden, gate_grad, up_grad, down_grad)


def solution(mesh):
    torus = Mesh(mesh.devices.reshape(NY, NX, NZ, 2), ("y", "x", "z", "c"))
    return jax.shard_map(
        on_device,
        mesh=torus,
        in_specs=(P(ROW, COL), P(ROW, COL), P(ROW), P(), P(ROW), P(ROW, COL), P(ROW, COL), P(ROW, COL)),
        out_specs=(P(ROW, COL), P(ROW, COL), P(ROW, COL), P(ROW, COL)),
        check_vma=False,
    )
```

```python
import jax
import jax.numpy as jnp
from jax import lax
from jax.experimental import pallas as pl
from jax.experimental.pallas import tpu as pltpu
from jax.sharding import Mesh
from jax.sharding import PartitionSpec as P

BLOCK = 128
WORK = 4
CAP = 6
NY, NX, NZ = 8, 4, 8
ROW = ("y", "x")
COL = ("z", "c")
NTAG = 16


def vmem():
    return pl.BlockSpec(memory_space=pltpu.VMEM)


def smem():
    return pl.BlockSpec(memory_space=pltpu.SMEM)


def params(**kw):
    return pltpu.CompilerParams(vmem_limit_bytes=60 * 1024 * 1024, **kw)


def move_count(moves):
    return moves.shape[1]


def pack_x(pos, moves, seg, tok, grad, box, work, masked):
    me = pos[0] * NX + pos[1]
    count = pos[2]
    span = WORK * BLOCK
    ids = seg[...]
    lane = lax.broadcasted_iota(jnp.int32, (CAP, BLOCK), 1)
    row = lax.broadcasted_iota(jnp.int32, (CAP, BLOCK), 0)
    ahead = jnp.concatenate([ids[1:], ids[-1:]], axis=0)
    joined = jnp.concatenate([ids[:, 1:], ahead[:, :1]], axis=1)
    mask = ((row * BLOCK + lane + 1 < count) & (joined == ids)).astype(jnp.float32)
    for b in range(CAP):
        rows = slice(b * BLOCK, (b + 1) * BLOCK)
        wide = jnp.broadcast_to(mask[b : b + 1, :], (BLOCK, BLOCK)).T
        masked[rows, :] = (grad[rows, :].astype(jnp.float32) * wide).astype(jnp.bfloat16)
    tally = jnp.sum(mask, axis=0, keepdims=True)
    for d in range(NX):
        box[d, 4 * BLOCK :, :] = jnp.broadcast_to(tally, (NTAG, BLOCK)).astype(jnp.bfloat16)

    def body(m, seen):
        src, dst, blk = moves[0, m], moves[1, m], moves[2, m]
        mine = src == me

        @pl.when(mine)
        def _():
            peer = dst % NX
            at = pl.multiple_of(seen * (2 * BLOCK), BLOCK)
            start = pl.multiple_of(blk * BLOCK, BLOCK)
            box[peer, pl.ds(at, BLOCK), :] = tok[pl.ds(start, BLOCK), :]
            box[peer, pl.ds(at + BLOCK, BLOCK), :] = masked[pl.ds(start, BLOCK), :]

        return jnp.where(mine, jnp.minimum(seen + 1, 1), seen)

    lax.fori_loop(0, move_count(moves), body, 0)
    work[0] = jnp.zeros_like(work[0])

    def own(b, nth):
        def gone(m, hit):
            return hit | ((moves[0, m] == me) & (moves[2, m] == b)).astype(jnp.int32)

        left = lax.fori_loop(0, move_count(moves), gone, 0)
        keep = (b * BLOCK < count) & (left == 0)

        @pl.when(keep & (nth < WORK))
        def _():
            start = pl.multiple_of(b * BLOCK, BLOCK)
            at = pl.multiple_of(nth * BLOCK, BLOCK)
            work[0, pl.ds(at, BLOCK), :] = tok[pl.ds(start, BLOCK), :]
            work[0, pl.ds(at + span, BLOCK), :] = masked[pl.ds(start, BLOCK), :]

        return nth + keep.astype(jnp.int32)

    lax.fori_loop(0, CAP, own, 0)
    for d in range(1, NZ):
        work[d] = work[0]


def pack_y(pos, moves, got, box, seen):
    my, mx = pos[0], pos[1]
    for i in range(NX):
        seen[i] = 0
    tally = got[0, 4 * BLOCK :, :].astype(jnp.float32)
    for i in range(1, NX):
        tally = tally + got[i, 4 * BLOCK :, :].astype(jnp.float32)
    for d in range(NY):
        box[d, 2 * BLOCK :, :] = tally.astype(jnp.bfloat16)

    def body(m, carry):
        src, dst = moves[0, m], moves[1, m]

        @pl.when(src // NX == my)
        def _():
            sx = src % NX
            nth = seen[sx]
            seen[sx] = jnp.minimum(nth + 1, 1)

            @pl.when(dst % NX == mx)
            def _():
                at = pl.multiple_of(nth * (2 * BLOCK), BLOCK)
                box[dst // NX, : 2 * BLOCK, :] = got[sx, pl.ds(at, 2 * BLOCK), :]

        return carry

    lax.fori_loop(0, move_count(moves), body, 0)


def pick_arrival(pos, moves, got, box, total):
    me = pos[0] * NX + pos[1]
    tally = got[0, 2 * BLOCK : 2 * BLOCK + 8, :].astype(jnp.float32)
    for i in range(1, NY):
        tally = tally + got[i, 2 * BLOCK : 2 * BLOCK + 8, :].astype(jnp.float32)
    total[...] = jnp.broadcast_to(jnp.sum(tally, axis=1, keepdims=True), total.shape)

    def came(m, at):
        return jnp.where(moves[1, m] == me, moves[0, m] // NX, at)

    sy = lax.fori_loop(0, move_count(moves), came, 0)
    for d in range(NZ):
        box[d] = got[sy, : 2 * BLOCK, :]


def compute(
    pos, moves, total, mine, other, late, late_other, wg, wu, wd,
    hidden, by_x, by_y, tok, grad, hid, back,
):
    j = pl.program_id(0)
    span = WORK * BLOCK
    tile = wg.shape[1]
    width = hid.shape[1]
    steps = width // tile

    @pl.when(j == 0)
    def _():
        me = pos[0] * NX + pos[1]
        first = pos[3] == 0
        for z in range(NZ):
            a, b = mine[z], other[z]
            low = jnp.where(first, a, b)
            high = jnp.where(first, b, a)
            at = z * 2 * BLOCK
            tok[:, at : at + BLOCK] = low[:span]
            grad[:, at : at + BLOCK] = low[span:]
            tok[:, at + BLOCK : at + 2 * BLOCK] = high[:span]
            grad[:, at + BLOCK : at + 2 * BLOCK] = high[span:]

        def own(b, nth):
            def gone(m, hit):
                return hit | ((moves[0, m] == me) & (moves[2, m] == b)).astype(jnp.int32)

            left = lax.fori_loop(0, move_count(moves), gone, 0)
            return nth + ((b * BLOCK < pos[2]) & (left == 0)).astype(jnp.int32)

        def came(m, hit):
            return hit | (moves[1, m] == me).astype(jnp.int32)

        nth = lax.fori_loop(0, CAP, own, 0)
        here = lax.fori_loop(0, move_count(moves), came, 0)

        @pl.when((here == 1) & (nth < WORK))
        def _():
            rows = pl.ds(pl.multiple_of(nth * BLOCK, BLOCK), BLOCK)
            for z in range(NZ):
                a, b = late[z], late_other[z]
                low = jnp.where(first, a, b)
                high = jnp.where(first, b, a)
                at = z * 2 * BLOCK
                tok[rows, at : at + BLOCK] = low[:BLOCK]
                grad[rows, at : at + BLOCK] = low[BLOCK:]
                tok[rows, at + BLOCK : at + 2 * BLOCK] = high[:BLOCK]
                grad[rows, at + BLOCK : at + 2 * BLOCK] = high[BLOCK:]

    for i in range(steps):

        @pl.when(j == i)
        def _():
            gate_sum = jnp.dot(tok[...], wg[...], preferred_element_type=jnp.float32)
            up_sum = jnp.dot(tok[...], wu[...], preferred_element_type=jnp.float32)
            back_sum = jnp.dot(grad[...], wd[...], preferred_element_type=jnp.float32)
            logistic = jax.nn.sigmoid(gate_sum)
            act = gate_sum * logistic
            value = (act * up_sum).astype(jnp.bfloat16)
            hidden[...] = value
            at = i * tile
            hid[:, at : at + tile] = value
            back[:, at : at + tile] = (
                back_sum * up_sum * logistic * (1.0 + gate_sum * (1.0 - logistic))
            ).astype(jnp.bfloat16)
            back[:, width + at : width + at + tile] = (back_sum * act).astype(jnp.bfloat16)

    for i in range(NY):

        @pl.when(j == steps + i)
        def _():
            inv = 1.0 / total[0, 0]
            per = by_x.shape[2]
            at = i * NX * per

            def term(left, right):
                out = lax.dot_general(
                    left, right, (((0,), (0,)), ((), ())), preferred_element_type=jnp.float32
                )
                return (out * inv).astype(jnp.bfloat16)

            both = term(tok[:, at : at + NX * per], back[...])
            for x in range(NX):
                by_x[x, 0] = both[x * per : (x + 1) * per, width:]
            by_y[0, :, :width] = both[:, :width]
            by_y[0, :, width:] = term(grad[:, at : at + NX * per], hid[...])


def add_x(got, out):
    acc = got[0].astype(jnp.float32)
    for i in range(1, NX):
        acc = acc + got[i].astype(jnp.float32)
    out[...] = acc.astype(jnp.bfloat16)


def finish(from_y, from_x, gate, up, down):
    acc = from_y[0].astype(jnp.float32)
    for i in range(1, NY):
        acc = acc + from_y[i].astype(jnp.float32)
    up[...] = acc
    bcc = from_x[0].astype(jnp.float32)
    for i in range(1, NX):
        bcc = bcc + from_x[i].astype(jnp.float32)
    width = gate.shape[1]
    gate[...] = bcc[:, :width]
    down[...] = bcc[:, width:]


def a2a(value, axis):
    return lax.all_to_all(value, axis, split_axis=0, concat_axis=0, tiled=True)


def swap(value):
    return lax.ppermute(value, "c", [(0, 1), (1, 0)])


def on_device(
    tokens, out_grad, counts, block_moves, segment_ids, gate_weight, up_weight, down_weight
):
    bf = jnp.bfloat16
    f32 = jnp.float32
    slots, feat = tokens.shape
    per, hid = gate_weight.shape
    span = WORK * BLOCK
    model = 2 * NZ * feat
    weights = lax.all_gather(
        jnp.concatenate([gate_weight, up_weight, down_weight], axis=1), ROW, axis=0, tiled=True
    )
    pos = jnp.stack([lax.axis_index("y"), lax.axis_index("x"), counts[0], lax.axis_index("c")])
    moves = block_moves.T
    box, work = pl.pallas_call(
        pack_x,
        out_shape=(
            jax.ShapeDtypeStruct((NX, 4 * BLOCK + NTAG, feat), bf),
            jax.ShapeDtypeStruct((NZ, 2 * span, feat), bf),
        ),
        in_specs=[smem(), smem(), vmem(), vmem(), vmem()],
        out_specs=(vmem(), vmem()),
        scratch_shapes=[pltpu.VMEM((slots, feat), bf)],
        compiler_params=params(),
        name="pack_x",
    )(pos, moves, segment_ids.reshape(CAP, BLOCK), tokens, out_grad)
    mine = a2a(work, "z")
    got = a2a(box, "x")
    box = pl.pallas_call(
        pack_y,
        out_shape=jax.ShapeDtypeStruct((NY, 2 * BLOCK + NTAG, feat), bf),
        in_specs=[smem(), smem(), vmem()],
        out_specs=vmem(),
        scratch_shapes=[pltpu.SMEM((NX,), jnp.int32)],
        compiler_params=params(),
        name="pack_y",
    )(pos, moves, got)
    got = a2a(box, "y")
    box, total = pl.pallas_call(
        pick_arrival,
        out_shape=(
            jax.ShapeDtypeStruct((NZ, 2 * BLOCK, feat), bf),
            jax.ShapeDtypeStruct((8, BLOCK), f32),
        ),
        in_specs=[smem(), smem(), vmem()],
        out_specs=(vmem(), vmem()),
        compiler_params=params(),
        name="pick_arrival",
    )(pos, moves, got)
    late = a2a(box, "z")
    other = swap(mine)
    late_other = swap(late)

    tile = 256
    steps = hid // tile

    def whole(shape):
        return pl.BlockSpec(shape, lambda j: (0,) * len(shape))

    def cols(rows, offset):
        return pl.BlockSpec((rows, tile), lambda j: (0, jnp.minimum(j, steps - 1) + offset))

    def later(j):
        return jnp.maximum(j - steps, 0)

    hidden, by_x, by_y = pl.pallas_call(
        compute,
        grid=(steps + NY,),
        out_shape=(
            jax.ShapeDtypeStruct((span, hid), bf),
            jax.ShapeDtypeStruct((NX, NY, per, hid), bf),
            jax.ShapeDtypeStruct((NY, NX * per, 2 * hid), bf),
        ),
        in_specs=[
            smem(),
            smem(),
            whole((8, BLOCK)),
            whole((NZ, 2 * span, feat)),
            whole((NZ, 2 * span, feat)),
            whole((NZ, 2 * BLOCK, feat)),
            whole((NZ, 2 * BLOCK, feat)),
            cols(model, 0),
            cols(model, steps),
            cols(model, 2 * steps),
        ],
        out_specs=(
            cols(span, 0),
            pl.BlockSpec((NX, 1, per, hid), lambda j: (0, later(j), 0, 0)),
            pl.BlockSpec((1, NX * per, 2 * hid), lambda j: (later(j), 0, 0)),
        ),
        scratch_shapes=[
            pltpu.VMEM((span, model), bf),
            pltpu.VMEM((span, model), bf),
            pltpu.VMEM((span, hid), bf),
            pltpu.VMEM((span, 2 * hid), bf),
        ],
        compiler_params=params(dimension_semantics=("arbitrary",)),
        name="compute",
    )(pos, moves, total, mine, other, late, late_other, weights, weights, weights)

    part_y = lax.psum_scatter(
        by_y.reshape(NY * NX * per, 2 * hid), "y", scatter_dimension=0, tiled=True
    )
    part_x = pl.pallas_call(
        add_x,
        out_shape=jax.ShapeDtypeStruct((NY, per, hid), bf),
        in_specs=[vmem()],
        out_specs=vmem(),
        compiler_params=params(),
        name="add_x",
    )(a2a(by_x, "x"))
    from_y = a2a(part_x, "y")
    from_x = a2a(part_y.reshape(NX, per, 2 * hid), "x")
    gate_grad, up_grad, down_grad = pl.pallas_call(
        finish,
        out_shape=tuple(jax.ShapeDtypeStruct((per, hid), f32) for _ in range(3)),
        in_specs=[vmem(), vmem()],
        out_specs=(vmem(), vmem(), vmem()),
        compiler_params=params(),
        name="finish",
    )(from_y, from_x)
    return (hidden, gate_grad, up_grad, down_grad)


def solution(mesh):
    torus = Mesh(mesh.devices.reshape(NY, NX, NZ, 2), ("y", "x", "z", "c"))
    return jax.shard_map(
        on_device,
        mesh=torus,
        in_specs=(P(ROW, COL), P(ROW, COL), P(ROW), P(), P(ROW), P(ROW, COL), P(ROW, COL), P(ROW, COL)),
        out_specs=(P(ROW, COL), P(ROW, COL), P(ROW, COL), P(ROW, COL)),
        check_vma=False,
    )
```

```python
import jax
import jax.numpy as jnp
from jax import lax
from jax.experimental import pallas as pl
from jax.experimental.pallas import tpu as pltpu
from jax.sharding import Mesh
from jax.sharding import PartitionSpec as P


BLOCK = 128
WORK = 4
CAP = 6
NY, NX, NZ = 8, 4, 8
ROW = ("y", "x")
COL = ("z", "c")
NTAG = 16


def vmem():
    return pl.BlockSpec(memory_space=pltpu.VMEM)


def smem():
    return pl.BlockSpec(memory_space=pltpu.SMEM)


def params(**kw):
    return pltpu.CompilerParams(vmem_limit_bytes=60 * 1024 * 1024, **kw)


def move_count(moves):
    return moves.shape[1]


def pack_x(pos, moves, seg, tok, grad, box, work, masked):
    me = pos[0] * NX + pos[1]
    count = pos[2]
    span = WORK * BLOCK
    ids = seg[...]
    lane = lax.broadcasted_iota(jnp.int32, (CAP, BLOCK), 1)
    row = lax.broadcasted_iota(jnp.int32, (CAP, BLOCK), 0)
    ahead = jnp.concatenate([ids[1:], ids[-1:]], axis=0)
    joined = jnp.concatenate([ids[:, 1:], ahead[:, :1]], axis=1)
    mask = ((row * BLOCK + lane + 1 < count) & (joined == ids)).astype(jnp.float32)
    for b in range(CAP):
        rows = slice(b * BLOCK, (b + 1) * BLOCK)
        wide = jnp.broadcast_to(mask[b : b + 1, :], (BLOCK, BLOCK)).T
        masked[rows, :] = (grad[rows, :].astype(jnp.float32) * wide).astype(jnp.bfloat16)
    tally = jnp.sum(mask, axis=0, keepdims=True)
    for d in range(NX):
        box[d, 4 * BLOCK :, :] = jnp.broadcast_to(tally, (NTAG, BLOCK)).astype(jnp.bfloat16)

    def body(m, seen):
        src, dst, blk = moves[0, m], moves[1, m], moves[2, m]
        mine = src == me

        @pl.when(mine)
        def _():
            peer = dst % NX
            at = pl.multiple_of(seen * (2 * BLOCK), BLOCK)
            start = pl.multiple_of(blk * BLOCK, BLOCK)
            box[peer, pl.ds(at, BLOCK), :] = tok[pl.ds(start, BLOCK), :]
            box[peer, pl.ds(at + BLOCK, BLOCK), :] = masked[pl.ds(start, BLOCK), :]

        return jnp.where(mine, jnp.minimum(seen + 1, 1), seen)

    lax.fori_loop(0, move_count(moves), body, 0)
    work[...] = jnp.zeros_like(work)

    def own(b, nth):
        def gone(m, hit):
            return hit | ((moves[0, m] == me) & (moves[2, m] == b)).astype(jnp.int32)

        left = lax.fori_loop(0, move_count(moves), gone, 0)
        keep = (b * BLOCK < count) & (left == 0)

        @pl.when(keep & (nth < WORK))
        def _():
            start = pl.multiple_of(b * BLOCK, BLOCK)
            at = pl.multiple_of(nth * BLOCK, BLOCK)
            work[pl.ds(at, BLOCK), :] = tok[pl.ds(start, BLOCK), :]
            work[pl.ds(at + span, BLOCK), :] = masked[pl.ds(start, BLOCK), :]

        return nth + keep.astype(jnp.int32)

    lax.fori_loop(0, CAP, own, 0)


def pack_y(pos, moves, got, box, seen):
    my, mx = pos[0], pos[1]
    for i in range(NX):
        seen[i] = 0
    tally = got[0, 4 * BLOCK :, :].astype(jnp.float32)
    for i in range(1, NX):
        tally = tally + got[i, 4 * BLOCK :, :].astype(jnp.float32)
    for d in range(NY):
        box[d, 2 * BLOCK :, :] = tally.astype(jnp.bfloat16)

    def body(m, carry):
        src, dst = moves[0, m], moves[1, m]

        @pl.when(src // NX == my)
        def _():
            sx = src % NX
            nth = seen[sx]
            seen[sx] = jnp.minimum(nth + 1, 1)

            @pl.when(dst % NX == mx)
            def _():
                at = pl.multiple_of(nth * (2 * BLOCK), BLOCK)
                box[dst // NX, : 2 * BLOCK, :] = got[sx, pl.ds(at, 2 * BLOCK), :]

        return carry

    lax.fori_loop(0, move_count(moves), body, 0)


def pick_arrival(pos, moves, got, box, total):
    me = pos[0] * NX + pos[1]
    tally = got[0, 2 * BLOCK : 2 * BLOCK + 8, :].astype(jnp.float32)
    for i in range(1, NY):
        tally = tally + got[i, 2 * BLOCK : 2 * BLOCK + 8, :].astype(jnp.float32)
    total[...] = jnp.broadcast_to(jnp.sum(tally, axis=1, keepdims=True), total.shape)

    def came(m, at):
        return jnp.where(moves[1, m] == me, moves[0, m] // NX, at)

    sy = lax.fori_loop(0, move_count(moves), came, 0)
    for d in range(NZ):
        box[d] = got[sy, : 2 * BLOCK, :]


def gather_up(*refs):
    out = refs[-1]
    for k, ref in enumerate(refs[:-1]):
        out[k] = ref[...]


def lay_out(pos, moves, mine, other, late, late_other, tok, grad, tok_t, grad_t):
    me = pos[0] * NX + pos[1]
    first = pos[3] == 0
    my_z = pos[4]
    span = WORK * BLOCK

    def own(b, nth):
        def gone(m, hit):
            return hit | ((moves[0, m] == me) & (moves[2, m] == b)).astype(jnp.int32)

        left = lax.fori_loop(0, move_count(moves), gone, 0)
        return nth + ((b * BLOCK < pos[2]) & (left == 0)).astype(jnp.int32)

    def came(m, hit):
        return hit | (moves[1, m] == me).astype(jnp.int32)

    nth = lax.fori_loop(0, CAP, own, 0)
    here = lax.fori_loop(0, move_count(moves), came, 0)
    there = (here == 1) & (nth < WORK)
    rows = pl.ds(pl.multiple_of(jnp.minimum(nth, WORK - 1) * BLOCK, BLOCK), BLOCK)
    for z in range(NZ):
        away = (my_z - z + NZ) % NZ
        a, b = mine[away], other[away]
        c, d = late[z], late_other[z]
        for side in range(2):
            cols = slice((2 * z + side) * BLOCK, (2 * z + side + 1) * BLOCK)
            take = first if side == 0 else jnp.logical_not(first)
            block = jnp.where(take, a, b)
            extra = jnp.where(take, c, d)
            tok[:, cols] = block[:span]
            grad[:, cols] = block[span:]

            @pl.when(there)
            def _():
                tok[rows, cols] = extra[:BLOCK]
                grad[rows, cols] = extra[BLOCK:]

            tok_t[cols, :] = tok[:, cols].T
            grad_t[cols, :] = grad[:, cols].T


def compute(total, tok, grad, wg, wu, wd, tok_t, grad_t, hidden, by_x, by_y, hid, back):
    j = pl.program_id(0)
    tile = wg.shape[1]
    width = hid.shape[1]
    steps = width // tile
    for i in range(steps):

        @pl.when(j == i)
        def _():
            gate_sum = jnp.dot(tok[...], wg[...], preferred_element_type=jnp.float32)
            up_sum = jnp.dot(tok[...], wu[...], preferred_element_type=jnp.float32)
            back_sum = jnp.dot(grad[...], wd[...], preferred_element_type=jnp.float32)
            logistic = jax.nn.sigmoid(gate_sum)
            act = gate_sum * logistic
            value = (act * up_sum).astype(jnp.bfloat16)
            hidden[...] = value
            at = i * tile
            hid[:, at : at + tile] = value
            back[:, at : at + tile] = (
                back_sum * up_sum * logistic * (1.0 + gate_sum * (1.0 - logistic))
            ).astype(jnp.bfloat16)
            back[:, width + at : width + at + tile] = (back_sum * act).astype(jnp.bfloat16)

    @pl.when(j >= steps)
    def _():
        inv = 1.0 / total[0, 0]
        per = by_x.shape[2]

        def term(left, right):
            out = jnp.dot(left, right, preferred_element_type=jnp.float32)
            return (out * inv).astype(jnp.bfloat16)

        both = term(tok_t[...], back[...])
        for x in range(NX):
            by_x[x, 0] = both[x * per : (x + 1) * per, width:]
        by_y[0, :, :width] = both[:, :width]
        by_y[0, :, width:] = term(grad_t[...], hid[...])


def add_x(got, out):
    acc = got[0].astype(jnp.float32)
    for i in range(1, NX):
        acc = acc + got[i].astype(jnp.float32)
    out[...] = acc.astype(jnp.bfloat16)


def finish(from_y, from_x, gate, up, down):
    acc = from_y[0].astype(jnp.float32)
    for i in range(1, NY):
        acc = acc + from_y[i].astype(jnp.float32)
    up[...] = acc
    bcc = from_x[0].astype(jnp.float32)
    for i in range(1, NX):
        bcc = bcc + from_x[i].astype(jnp.float32)
    width = gate.shape[1]
    gate[...] = bcc[:, :width]
    down[...] = bcc[:, width:]


def a2a(value, axis):
    return lax.all_to_all(value, axis, split_axis=0, concat_axis=0, tiled=True)


def swap(value):
    return lax.ppermute(value, "c", [(0, 1), (1, 0)])


def along_z(value, by):
    return lax.ppermute(value, "z", [(i, (i + by) % NZ) for i in range(NZ)])


def on_device(
    tokens, out_grad, counts, block_moves, segment_ids, gate_weight, up_weight, down_weight
):
    bf = jnp.bfloat16
    f32 = jnp.float32
    slots, feat = tokens.shape
    per, hid = gate_weight.shape
    span = WORK * BLOCK
    model = 2 * NZ * feat
    weights = lax.all_gather(
        jnp.concatenate([gate_weight, up_weight, down_weight], axis=1), ROW, axis=0, tiled=True
    )
    pos = jnp.stack([lax.axis_index("y"), lax.axis_index("x"), counts[0], lax.axis_index("c"), lax.axis_index("z")])
    moves = block_moves.T
    box, work = pl.pallas_call(
        pack_x,
        out_shape=(
            jax.ShapeDtypeStruct((NX, 4 * BLOCK + NTAG, feat), bf),
            jax.ShapeDtypeStruct((2 * span, feat), bf),
        ),
        in_specs=[smem(), smem(), vmem(), vmem(), vmem()],
        out_specs=(vmem(), vmem()),
        scratch_shapes=[pltpu.VMEM((slots, feat), bf)],
        compiler_params=params(),
        name="pack_x",
    )(pos, moves, segment_ids.reshape(CAP, BLOCK), tokens, out_grad)
    up1, down1 = along_z(work, 1), along_z(work, -1)
    up2, down2 = along_z(work, 2), along_z(work, -2)
    up3, down3, up4 = along_z(up2, 1), along_z(down2, -1), along_z(up2, 2)
    got = a2a(box, "x")
    box = pl.pallas_call(
        pack_y,
        out_shape=jax.ShapeDtypeStruct((NY, 2 * BLOCK + NTAG, feat), bf),
        in_specs=[smem(), smem(), vmem()],
        out_specs=vmem(),
        scratch_shapes=[pltpu.SMEM((NX,), jnp.int32)],
        compiler_params=params(),
        name="pack_y",
    )(pos, moves, got)
    got = a2a(box, "y")
    box, total = pl.pallas_call(
        pick_arrival,
        out_shape=(
            jax.ShapeDtypeStruct((NZ, 2 * BLOCK, feat), bf),
            jax.ShapeDtypeStruct((8, BLOCK), f32),
        ),
        in_specs=[smem(), smem(), vmem()],
        out_specs=(vmem(), vmem()),
        compiler_params=params(),
        name="pick_arrival",
    )(pos, moves, got)
    late = a2a(box, "z")
    pieces = (work, up1, up2, up3, up4, down3, down2, down1)
    mine = pl.pallas_call(
        gather_up,
        out_shape=jax.ShapeDtypeStruct((NZ, 2 * span, feat), bf),
        in_specs=[vmem()] * NZ,
        out_specs=vmem(),
        compiler_params=params(),
        name="gather_up",
    )(*pieces)
    other = swap(mine)
    late_other = swap(late)

    tile = 256
    steps = hid // tile

    def whole(shape):
        return pl.BlockSpec(shape, lambda j: (0,) * len(shape))

    def cols(rows, offset):
        return pl.BlockSpec((rows, tile), lambda j: (0, jnp.minimum(j, steps - 1) + offset))

    def later(j):
        return jnp.maximum(j - steps, 0)

    tok, grad, tok_t, grad_t = pl.pallas_call(
        lay_out,
        out_shape=(
            jax.ShapeDtypeStruct((span, model), bf),
            jax.ShapeDtypeStruct((span, model), bf),
            jax.ShapeDtypeStruct((model, span), bf),
            jax.ShapeDtypeStruct((model, span), bf),
        ),
        in_specs=[smem(), smem(), vmem(), vmem(), vmem(), vmem()],
        out_specs=(vmem(),) * 4,
        compiler_params=params(),
        name="lay_out",
    )(pos, moves, mine, other, late, late_other)

    hidden, by_x, by_y = pl.pallas_call(
        compute,
        grid=(steps + NY,),
        out_shape=(
            jax.ShapeDtypeStruct((span, hid), bf),
            jax.ShapeDtypeStruct((NX, NY, per, hid), bf),
            jax.ShapeDtypeStruct((NY, NX * per, 2 * hid), bf),
        ),
        in_specs=[
            whole((8, BLOCK)),
            whole((span, model)),
            whole((span, model)),
            cols(model, 0),
            cols(model, steps),
            cols(model, 2 * steps),
            pl.BlockSpec((NX * per, span), lambda j: (later(j), 0)),
            pl.BlockSpec((NX * per, span), lambda j: (later(j), 0)),
        ],
        out_specs=(
            cols(span, 0),
            pl.BlockSpec((NX, 1, per, hid), lambda j: (0, later(j), 0, 0)),
            pl.BlockSpec((1, NX * per, 2 * hid), lambda j: (later(j), 0, 0)),
        ),
        scratch_shapes=[pltpu.VMEM((span, hid), bf), pltpu.VMEM((span, 2 * hid), bf)],
        compiler_params=params(dimension_semantics=("arbitrary",)),
        name="compute",
    )(total, tok, grad, weights, weights, weights, tok_t, grad_t)

    part_y = lax.psum_scatter(
        by_y.reshape(NY * NX * per, 2 * hid), "y", scatter_dimension=0, tiled=True
    )
    part_x = pl.pallas_call(
        add_x,
        out_shape=jax.ShapeDtypeStruct((NY, per, hid), bf),
        in_specs=[vmem()],
        out_specs=vmem(),
        compiler_params=params(),
        name="add_x",
    )(a2a(by_x, "x"))
    from_y = a2a(part_x, "y")
    from_x = a2a(part_y.reshape(NX, per, 2 * hid), "x")
    gate_grad, up_grad, down_grad = pl.pallas_call(
        finish,
        out_shape=tuple(jax.ShapeDtypeStruct((per, hid), f32) for _ in range(3)),
        in_specs=[vmem(), vmem()],
        out_specs=(vmem(), vmem(), vmem()),
        compiler_params=params(),
        name="finish",
    )(from_y, from_x)
    return (hidden, gate_grad, up_grad, down_grad)


def solution(mesh):
    torus = Mesh(mesh.devices.reshape(NY, NX, NZ, 2), ("y", "x", "z", "c"))
    return jax.shard_map(
        on_device,
        mesh=torus,
        in_specs=(P(ROW, COL), P(ROW, COL), P(ROW), P(), P(ROW), P(ROW, COL), P(ROW, COL), P(ROW, COL)),
        out_specs=(P(ROW, COL), P(ROW, COL), P(ROW, COL), P(ROW, COL)),
        check_vma=False,
    )
```

```python
import jax
import jax.numpy as jnp
from jax import lax
from jax.experimental import pallas as pl
from jax.experimental.pallas import tpu as pltpu
from jax.sharding import Mesh
from jax.sharding import PartitionSpec as P


BLOCK = 128
WORK = 4
CAP = 6
NY, NX, NZ = 8, 4, 8
ROW = ("y", "x")
COL = ("z", "c")
NTAG = 16
CUT = 128


def vmem():
    return pl.BlockSpec(memory_space=pltpu.VMEM)


def smem():
    return pl.BlockSpec(memory_space=pltpu.SMEM)


def params(mib, **kw):
    return pltpu.CompilerParams(vmem_limit_bytes=mib * 1024 * 1024, **kw)


def move_count(moves):
    return moves.shape[1]


def pack_x(pos, moves, seg, tok, grad, box, work, masked):
    me = pos[0] * NX + pos[1]
    count = pos[2]
    span = WORK * BLOCK
    ids = seg[...]
    lane = lax.broadcasted_iota(jnp.int32, (CAP, BLOCK), 1)
    row = lax.broadcasted_iota(jnp.int32, (CAP, BLOCK), 0)
    ahead = jnp.concatenate([ids[1:], ids[-1:]], axis=0)
    joined = jnp.concatenate([ids[:, 1:], ahead[:, :1]], axis=1)
    mask = ((row * BLOCK + lane + 1 < count) & (joined == ids)).astype(jnp.float32)
    for b in range(CAP):
        rows = slice(b * BLOCK, (b + 1) * BLOCK)
        wide = jnp.broadcast_to(mask[b : b + 1, :], (BLOCK, BLOCK)).T
        masked[rows, :] = (grad[rows, :].astype(jnp.float32) * wide).astype(jnp.bfloat16)
    tally = jnp.sum(mask, axis=0, keepdims=True)
    for d in range(NX):
        box[d, 4 * BLOCK :, :] = jnp.broadcast_to(tally, (NTAG, BLOCK)).astype(jnp.bfloat16)

    def body(m, seen):
        src, dst, blk = moves[0, m], moves[1, m], moves[2, m]
        mine = src == me

        @pl.when(mine)
        def _():
            peer = dst % NX
            at = pl.multiple_of(seen * (2 * BLOCK), BLOCK)
            start = pl.multiple_of(blk * BLOCK, BLOCK)
            box[peer, pl.ds(at, BLOCK), :] = tok[pl.ds(start, BLOCK), :]
            box[peer, pl.ds(at + BLOCK, BLOCK), :] = masked[pl.ds(start, BLOCK), :]

        return jnp.where(mine, jnp.minimum(seen + 1, 1), seen)

    lax.fori_loop(0, move_count(moves), body, 0)
    work[...] = jnp.zeros_like(work)

    def own(b, nth):
        def gone(m, hit):
            return hit | ((moves[0, m] == me) & (moves[2, m] == b)).astype(jnp.int32)

        left = lax.fori_loop(0, move_count(moves), gone, 0)
        keep = (b * BLOCK < count) & (left == 0)

        @pl.when(keep & (nth < WORK))
        def _():
            start = pl.multiple_of(b * BLOCK, BLOCK)
            at = pl.multiple_of(nth * BLOCK, BLOCK)
            work[pl.ds(at, BLOCK), :] = tok[pl.ds(start, BLOCK), :]
            work[pl.ds(at + span, BLOCK), :] = masked[pl.ds(start, BLOCK), :]

        return nth + keep.astype(jnp.int32)

    lax.fori_loop(0, CAP, own, 0)


def pack_y(pos, moves, got, box, seen):
    my, mx = pos[0], pos[1]
    for i in range(NX):
        seen[i] = 0
    tally = got[0, 4 * BLOCK :, :].astype(jnp.float32)
    for i in range(1, NX):
        tally = tally + got[i, 4 * BLOCK :, :].astype(jnp.float32)
    for d in range(NY):
        box[d, 2 * BLOCK :, :] = tally.astype(jnp.bfloat16)

    def body(m, carry):
        src, dst = moves[0, m], moves[1, m]

        @pl.when(src // NX == my)
        def _():
            sx = src % NX
            nth = seen[sx]
            seen[sx] = jnp.minimum(nth + 1, 1)

            @pl.when(dst % NX == mx)
            def _():
                at = pl.multiple_of(nth * (2 * BLOCK), BLOCK)
                box[dst // NX, : 2 * BLOCK, :] = got[sx, pl.ds(at, 2 * BLOCK), :]

        return carry

    lax.fori_loop(0, move_count(moves), body, 0)


def pick_arrival(pos, moves, got, box, total):
    me = pos[0] * NX + pos[1]
    tally = got[0, 2 * BLOCK : 2 * BLOCK + 8, :].astype(jnp.float32)
    for i in range(1, NY):
        tally = tally + got[i, 2 * BLOCK : 2 * BLOCK + 8, :].astype(jnp.float32)
    total[...] = jnp.broadcast_to(jnp.sum(tally, axis=1, keepdims=True), total.shape)

    def came(m, at):
        return jnp.where(moves[1, m] == me, moves[0, m] // NX, at)

    sy = lax.fori_loop(0, move_count(moves), came, 0)
    for d in range(NZ):
        box[d] = got[sy, : 2 * BLOCK, :]


def gather_up(pos, *refs):
    pieces, late, out = refs[:NZ], refs[NZ], refs[NZ + 1]
    rows = pieces[0].shape[0]
    for k, piece in enumerate(pieces):
        out[k, :rows, :] = piece[...]
        out[k, rows:, :] = late[(pos[4] - k + NZ) % NZ]


def lay_out(pos, moves, mine, other, tok, grad):
    me = pos[0] * NX + pos[1]
    first = pos[3] == 0
    my_z = pos[4]
    span = WORK * BLOCK

    def own(b, nth):
        def gone(m, hit):
            return hit | ((moves[0, m] == me) & (moves[2, m] == b)).astype(jnp.int32)

        left = lax.fori_loop(0, move_count(moves), gone, 0)
        return nth + ((b * BLOCK < pos[2]) & (left == 0)).astype(jnp.int32)

    def came(m, hit):
        return hit | (moves[1, m] == me).astype(jnp.int32)

    nth = lax.fori_loop(0, CAP, own, 0)
    here = lax.fori_loop(0, move_count(moves), came, 0)

    def pick(z, side, low, size):
        away = (my_z - z + NZ) % NZ
        take = first if side == 0 else jnp.logical_not(first)
        rows = slice(low, low + size)
        return jnp.where(take, mine[away, rows, :], other[away, rows, :])

    for z in range(NZ):
        for side in range(2):
            cols = slice((2 * z + side) * BLOCK, (2 * z + side + 1) * BLOCK)
            tok[:, cols] = pick(z, side, 0, span)
            grad[:, cols] = pick(z, side, span, span)

    @pl.when((here == 1) & (nth < WORK))
    def _():
        rows = pl.ds(pl.multiple_of(nth * BLOCK, BLOCK), BLOCK)
        for z in range(NZ):
            for side in range(2):
                cols = slice((2 * z + side) * BLOCK, (2 * z + side + 1) * BLOCK)
                tok[rows, cols] = pick(z, side, 2 * span, BLOCK)
                grad[rows, cols] = pick(z, side, 2 * span + BLOCK, BLOCK)


def compute(
    total, tok_in, grad_in, weights, hidden, by_x, by_y,
    tok, grad, held, hid, back, stage, in_sem, out_sem, hid_sem,
):
    width = hid.shape[1]
    tile = width // 2
    per = by_x.shape[2]
    cut = by_x.shape[3] - width
    loads = (
        pltpu.make_async_copy(tok_in, tok, in_sem.at[0]),
        pltpu.make_async_copy(grad_in, grad, in_sem.at[1]),
        pltpu.make_async_copy(weights, held, in_sem.at[2]),
    )
    for load in loads:
        load.start()
    for load in loads:
        load.wait()
    for at in range(0, width, tile):
        gate_w, up_w, down_w = (held[:, k * width + at : k * width + at + tile] for k in range(3))
        gate_sum = jnp.dot(tok[...], gate_w, preferred_element_type=jnp.float32)
        up_sum = jnp.dot(tok[...], up_w, preferred_element_type=jnp.float32)
        back_sum = jnp.dot(grad[...], down_w, preferred_element_type=jnp.float32)
        logistic = jax.nn.sigmoid(gate_sum)
        act = gate_sum * logistic
        hid[:, at : at + tile] = (act * up_sum).astype(jnp.bfloat16)
        back[:, at : at + tile] = (
            back_sum * up_sum * logistic * (1.0 + gate_sum * (1.0 - logistic))
        ).astype(jnp.bfloat16)
        back[:, width + at : width + at + tile] = (back_sum * act).astype(jnp.bfloat16)
    keep = pltpu.make_async_copy(hid, hidden, hid_sem)
    keep.start()
    inv = 1.0 / total[0, 0]

    def term(left, right):
        out = lax.dot_general(
            left, right, (((0,), (0,)), ((), ())), preferred_element_type=jnp.float32
        )
        return (out * inv).astype(jnp.bfloat16)

    stores = []
    for y in range(NY):
        at = y * NX * per
        both = term(tok[:, at : at + NX * per], back[...])
        for x in range(NX):
            by_x[x, y, :, :width] = both[x * per : (x + 1) * per, width:]
            by_x[x, y, :, width:] = both[x * per : (x + 1) * per, :cut]
        stage[y, :, : width - cut] = both[:, cut:width]
        stage[y, :, width - cut :] = term(grad[:, at : at + NX * per], hid[...])
        stores.append(pltpu.make_async_copy(stage.at[y], by_y.at[y], out_sem.at[y]))
        stores[y].start()
    for store in stores:
        store.wait()
    keep.wait()


def add_x(got, out):
    acc = got[0].astype(jnp.float32)
    for i in range(1, NX):
        acc = acc + got[i].astype(jnp.float32)
    out[...] = acc.astype(jnp.bfloat16)


def turn(pos, part, *outs):
    for k, out in enumerate(outs):
        out[...] = part[(pos[1] + k) % NX]


def finish(from_y, *refs):
    parts, (gate, up, down) = refs[:NX], refs[NX:]
    acc = from_y[0].astype(jnp.float32)
    for i in range(1, NY):
        acc = acc + from_y[i].astype(jnp.float32)
    bcc = parts[0][...].astype(jnp.float32)
    for part in parts[1:]:
        bcc = bcc + part[...].astype(jnp.float32)
    width = up.shape[1]
    cut = acc.shape[1] - width
    up[...] = acc[:, :width]
    gate[:, :cut] = acc[:, width:]
    gate[:, cut:] = bcc[:, : width - cut]
    down[...] = bcc[:, width - cut :]


def a2a(value, axis):
    return lax.all_to_all(value, axis, split_axis=0, concat_axis=0, tiled=True)


def swap(value):
    return lax.ppermute(value, "c", [(0, 1), (1, 0)])


def along_z(value, by):
    return lax.ppermute(value, "z", [(i, (i + by) % NZ) for i in range(NZ)])


def step(
    tokens, out_grad, counts, block_moves, segment_ids, gate_weight, up_weight, down_weight
):
    bf = jnp.bfloat16
    f32 = jnp.float32
    slots, feat = tokens.shape
    per, hid = gate_weight.shape
    span = WORK * BLOCK
    model = 2 * NZ * feat
    weights = lax.all_gather(
        jnp.concatenate([gate_weight, up_weight, down_weight], axis=1), ROW, axis=0, tiled=True
    )
    pos = jnp.stack([lax.axis_index("y"), lax.axis_index("x"), counts[0], lax.axis_index("c"), lax.axis_index("z")])
    moves = block_moves.T
    box, work = pl.pallas_call(
        pack_x,
        out_shape=(
            jax.ShapeDtypeStruct((NX, 4 * BLOCK + NTAG, feat), bf),
            jax.ShapeDtypeStruct((2 * span, feat), bf),
        ),
        in_specs=[smem(), smem(), vmem(), vmem(), vmem()],
        out_specs=(vmem(), vmem()),
        scratch_shapes=[pltpu.VMEM((slots, feat), bf)],
        compiler_params=params(8),
        name="pack_x",
    )(pos, moves, segment_ids.reshape(CAP, BLOCK), tokens, out_grad)
    up2, down2 = along_z(work, 2), along_z(work, -2)
    up1, down1 = along_z(work, 1), along_z(work, -1)
    up3, down3, up4 = along_z(up2, 1), along_z(down2, -1), along_z(up2, 2)
    got = a2a(box, "x")
    box = pl.pallas_call(
        pack_y,
        out_shape=jax.ShapeDtypeStruct((NY, 2 * BLOCK + NTAG, feat), bf),
        in_specs=[smem(), smem(), vmem()],
        out_specs=vmem(),
        scratch_shapes=[pltpu.SMEM((NX,), jnp.int32)],
        compiler_params=params(8),
        name="pack_y",
    )(pos, moves, got)
    got = a2a(box, "y")
    box, total = pl.pallas_call(
        pick_arrival,
        out_shape=(
            jax.ShapeDtypeStruct((NZ, 2 * BLOCK, feat), bf),
            jax.ShapeDtypeStruct((8, BLOCK), f32),
        ),
        in_specs=[smem(), smem(), vmem()],
        out_specs=(vmem(), vmem()),
        compiler_params=params(8),
        name="pick_arrival",
    )(pos, moves, got)
    late = a2a(box, "z")
    pieces = (work, up1, up2, up3, up4, down3, down2, down1)
    mine = pl.pallas_call(
        gather_up,
        out_shape=jax.ShapeDtypeStruct((NZ, 2 * span + 2 * BLOCK, feat), bf),
        in_specs=[smem()] + [vmem()] * (NZ + 1),
        out_specs=vmem(),
        compiler_params=params(12),
        name="gather_up",
    )(pos, *pieces, late)
    other = swap(mine)
    tok, grad = pl.pallas_call(
        lay_out,
        out_shape=(
            jax.ShapeDtypeStruct((span, model), bf),
            jax.ShapeDtypeStruct((span, model), bf),
        ),
        in_specs=[smem(), smem(), vmem(), vmem()],
        out_specs=(vmem(), vmem()),
        compiler_params=params(14),
        name="lay_out",
    )(pos, moves, mine, other)

    hbm = pl.BlockSpec(memory_space=pltpu.HBM)
    wide_x, wide_y = hid + CUT, 2 * hid - CUT
    hidden, by_x, by_y = pl.pallas_call(
        compute,
        out_shape=(
            pltpu.HBM((span, hid), bf),
            pltpu.VMEM((NX, NY, per, wide_x), bf),
            pltpu.HBM((NY, NX * per, wide_y), bf),
        ),
        in_specs=[vmem(), hbm, hbm, hbm],
        out_specs=(hbm, vmem(), hbm),
        scratch_shapes=[
            pltpu.VMEM((span, model), bf),
            pltpu.VMEM((span, model), bf),
            pltpu.VMEM((model, 3 * hid), bf),
            pltpu.VMEM((span, hid), bf),
            pltpu.VMEM((span, 2 * hid), bf),
            pltpu.VMEM((NY, NX * per, wide_y), bf),
            pltpu.SemaphoreType.DMA((3,)),
            pltpu.SemaphoreType.DMA((NY,)),
            pltpu.SemaphoreType.DMA(()),
        ],
        compiler_params=params(36),
        name="compute",
    )(
        total,
        pltpu.with_memory_space_constraint(tok, pltpu.HBM),
        pltpu.with_memory_space_constraint(grad, pltpu.HBM),
        pltpu.with_memory_space_constraint(weights, pltpu.HBM),
    )

    part_y = lax.psum_scatter(
        by_y.reshape(NY * NX * per, wide_y), "y", scatter_dimension=0, tiled=True
    )
    part_x = pl.pallas_call(
        add_x,
        out_shape=jax.ShapeDtypeStruct((NY, per, wide_x), bf),
        in_specs=[vmem()],
        out_specs=vmem(),
        compiler_params=params(8),
        name="add_x",
    )(a2a(by_x, "x"))
    from_y = a2a(part_x, "y")
    turned = pl.pallas_call(
        turn,
        out_shape=tuple(jax.ShapeDtypeStruct((per, wide_y), bf) for _ in range(NX)),
        in_specs=[smem(), vmem()],
        out_specs=(vmem(),) * NX,
        compiler_params=params(8),
        name="turn",
    )(pos, part_y.reshape(NX, per, wide_y))
    from_x = [turned[0]] + [
        lax.ppermute(turned[k], "x", [(i, (i + k) % NX) for i in range(NX)]) for k in range(1, NX)
    ]
    gate_grad, up_grad, down_grad = pl.pallas_call(
        finish,
        out_shape=tuple(jax.ShapeDtypeStruct((per, hid), f32) for _ in range(3)),
        in_specs=[vmem()] * (NX + 1),
        out_specs=(vmem(), vmem(), vmem()),
        compiler_params=params(8),
        name="finish",
    )(from_y, *from_x)
    return (hidden, gate_grad, up_grad, down_grad)


def solution(mesh):
    torus = Mesh(mesh.devices.reshape(NY, NX, NZ, 2), ("y", "x", "z", "c"))
    return jax.shard_map(
        step,
        mesh=torus,
        in_specs=(P(ROW, COL), P(ROW, COL), P(ROW), P(), P(ROW), P(ROW, COL), P(ROW, COL), P(ROW, COL)),
        out_specs=(P(ROW, COL), P(ROW, COL), P(ROW, COL), P(ROW, COL)),
        check_vma=False,
    )
```

```python
import jax
import jax.numpy as jnp
from jax import lax
from jax.experimental import pallas as pl
from jax.experimental.pallas import tpu as pltpu
from jax.sharding import Mesh
from jax.sharding import PartitionSpec as P


BLOCK = 128
WORK = 4
CAP = 6
NY, NX, NZ = 8, 4, 8
ROW = ("y", "x")
COL = ("z", "c")
NTAG = 16
CUT = 256


def vmem():
    return pl.BlockSpec(memory_space=pltpu.VMEM)


def smem():
    return pl.BlockSpec(memory_space=pltpu.SMEM)


def params(mib, **kw):
    return pltpu.CompilerParams(vmem_limit_bytes=mib * 1024 * 1024, **kw)


def move_count(moves):
    return moves.shape[1]


def pack_x(pos, moves, seg, tok, grad, box, work, masked):
    me = pos[0] * NX + pos[1]
    count = pos[2]
    span = WORK * BLOCK
    ids = seg[...]
    lane = lax.broadcasted_iota(jnp.int32, (CAP, BLOCK), 1)
    row = lax.broadcasted_iota(jnp.int32, (CAP, BLOCK), 0)
    ahead = jnp.concatenate([ids[1:], ids[-1:]], axis=0)
    joined = jnp.concatenate([ids[:, 1:], ahead[:, :1]], axis=1)
    mask = ((row * BLOCK + lane + 1 < count) & (joined == ids)).astype(jnp.float32)
    for b in range(CAP):
        rows = slice(b * BLOCK, (b + 1) * BLOCK)
        wide = jnp.broadcast_to(mask[b : b + 1, :], (BLOCK, BLOCK)).T
        masked[rows, :] = (grad[rows, :].astype(jnp.float32) * wide).astype(jnp.bfloat16)
    tally = jnp.sum(mask, axis=0, keepdims=True)
    for d in range(NX):
        box[d, 4 * BLOCK :, :] = jnp.broadcast_to(tally, (NTAG, BLOCK)).astype(jnp.bfloat16)

    def body(m, seen):
        src, dst, blk = moves[0, m], moves[1, m], moves[2, m]
        mine = src == me

        @pl.when(mine)
        def _():
            peer = dst % NX
            at = pl.multiple_of(seen * (2 * BLOCK), BLOCK)
            start = pl.multiple_of(blk * BLOCK, BLOCK)
            box[peer, pl.ds(at, BLOCK), :] = tok[pl.ds(start, BLOCK), :]
            box[peer, pl.ds(at + BLOCK, BLOCK), :] = masked[pl.ds(start, BLOCK), :]

        return jnp.where(mine, jnp.minimum(seen + 1, 1), seen)

    lax.fori_loop(0, move_count(moves), body, 0)
    work[...] = jnp.zeros_like(work)

    def own(b, nth):
        def gone(m, hit):
            return hit | ((moves[0, m] == me) & (moves[2, m] == b)).astype(jnp.int32)

        left = lax.fori_loop(0, move_count(moves), gone, 0)
        keep = (b * BLOCK < count) & (left == 0)

        @pl.when(keep & (nth < WORK))
        def _():
            start = pl.multiple_of(b * BLOCK, BLOCK)
            at = pl.multiple_of(nth * BLOCK, BLOCK)
            work[pl.ds(at, BLOCK), :] = tok[pl.ds(start, BLOCK), :]
            work[pl.ds(at + span, BLOCK), :] = masked[pl.ds(start, BLOCK), :]

        return nth + keep.astype(jnp.int32)

    lax.fori_loop(0, CAP, own, 0)


def pack_y(pos, moves, got, box, seen):
    my, mx = pos[0], pos[1]
    for i in range(NX):
        seen[i] = 0
    tally = got[0, 4 * BLOCK :, :].astype(jnp.float32)
    for i in range(1, NX):
        tally = tally + got[i, 4 * BLOCK :, :].astype(jnp.float32)
    for d in range(NY):
        box[d, 2 * BLOCK :, :] = tally.astype(jnp.bfloat16)

    def body(m, carry):
        src, dst = moves[0, m], moves[1, m]

        @pl.when(src // NX == my)
        def _():
            sx = src % NX
            nth = seen[sx]
            seen[sx] = jnp.minimum(nth + 1, 1)

            @pl.when(dst % NX == mx)
            def _():
                at = pl.multiple_of(nth * (2 * BLOCK), BLOCK)
                box[dst // NX, : 2 * BLOCK, :] = got[sx, pl.ds(at, 2 * BLOCK), :]

        return carry

    lax.fori_loop(0, move_count(moves), body, 0)


def pick_arrival(pos, moves, got, box, total):
    me = pos[0] * NX + pos[1]
    tally = got[0, 2 * BLOCK : 2 * BLOCK + 8, :].astype(jnp.float32)
    for i in range(1, NY):
        tally = tally + got[i, 2 * BLOCK : 2 * BLOCK + 8, :].astype(jnp.float32)
    total[...] = jnp.broadcast_to(jnp.sum(tally, axis=1, keepdims=True), total.shape)

    def came(m, at):
        return jnp.where(moves[1, m] == me, moves[0, m] // NX, at)

    sy = lax.fori_loop(0, move_count(moves), came, 0)
    for d in range(NZ):
        box[d] = got[sy, : 2 * BLOCK, :]


def gather_up(*refs):
    out = refs[-1]
    for k, piece in enumerate(refs[:-1]):
        out[k] = piece[...]


def lay_out(pos, moves, mine, other, late, late_other, tok_out, grad_out, tok, grad, sems):
    me = pos[0] * NX + pos[1]
    first = pos[3] == 0
    my_z = pos[4]
    span = WORK * BLOCK

    def own(b, nth):
        def gone(m, hit):
            return hit | ((moves[0, m] == me) & (moves[2, m] == b)).astype(jnp.int32)

        left = lax.fori_loop(0, move_count(moves), gone, 0)
        return nth + ((b * BLOCK < pos[2]) & (left == 0)).astype(jnp.int32)

    def came(m, hit):
        return hit | (moves[1, m] == me).astype(jnp.int32)

    nth = lax.fori_loop(0, CAP, own, 0)
    here = lax.fori_loop(0, move_count(moves), came, 0)
    there = (here == 1) & (nth < WORK)
    rows = pl.ds(pl.multiple_of(jnp.minimum(nth, WORK - 1) * BLOCK, BLOCK), BLOCK)
    sends = []
    for z in range(NZ):
        away = (my_z - z + NZ) % NZ
        for side in range(2):
            cols = slice((2 * z + side) * BLOCK, (2 * z + side + 1) * BLOCK)
            take = first if side == 0 else jnp.logical_not(first)
            block = jnp.where(take, mine[away], other[away])
            tok[:, cols] = block[:span]
            grad[:, cols] = block[span:]

            @pl.when(there)
            def _():
                extra = jnp.where(take, late[z], late_other[z])
                tok[rows, cols] = extra[:BLOCK]
                grad[rows, cols] = extra[BLOCK:]

        both = slice(2 * z * BLOCK, 2 * (z + 1) * BLOCK)
        for k, (ref, out) in enumerate(((tok, tok_out), (grad, grad_out))):
            sends.append(pltpu.make_async_copy(ref.at[:, both], out.at[:, both], sems.at[k, z]))
            sends[-1].start()
    for send in sends:
        send.wait()


def compute(
    total, tok_in, grad_in, weights, hidden, by_x, by_y,
    tok, grad, held, hid, back, stage, in_sem, out_sem, hid_sem,
):
    width = hid.shape[1]
    tile = width // 2
    per = by_x.shape[2]
    cut = by_x.shape[3] - width
    fore = 2 * width
    loads = (
        pltpu.make_async_copy(tok_in, tok, in_sem.at[0]),
        pltpu.make_async_copy(weights.at[:, :fore], held.at[:, :fore], in_sem.at[1]),
        pltpu.make_async_copy(grad_in, grad, in_sem.at[2]),
        pltpu.make_async_copy(weights.at[:, fore:], held.at[:, fore:], in_sem.at[3]),
    )
    for load in loads:
        load.start()
    loads[0].wait()
    loads[1].wait()
    sums = jnp.dot(tok[...], held[:, :fore], preferred_element_type=jnp.float32)
    loads[2].wait()
    loads[3].wait()
    for at in range(0, width, tile):
        gate_sum = sums[:, at : at + tile]
        up_sum = sums[:, width + at : width + at + tile]
        down_w = held[:, fore + at : fore + at + tile]
        back_sum = jnp.dot(grad[...], down_w, preferred_element_type=jnp.float32)
        logistic = jax.nn.sigmoid(gate_sum)
        act = gate_sum * logistic
        hid[:, at : at + tile] = (act * up_sum).astype(jnp.bfloat16)
        back[:, at : at + tile] = (
            back_sum * up_sum * logistic * (1.0 + gate_sum * (1.0 - logistic))
        ).astype(jnp.bfloat16)
        back[:, width + at : width + at + tile] = (back_sum * act).astype(jnp.bfloat16)
    keep = pltpu.make_async_copy(hid, hidden, hid_sem)
    keep.start()
    inv = 1.0 / total[0, 0]

    def term(left, right):
        out = lax.dot_general(
            left, right, (((0,), (0,)), ((), ())), preferred_element_type=jnp.float32
        )
        return (out * inv).astype(jnp.bfloat16)

    stores = []
    for y in range(NY):
        at = y * NX * per
        both = term(tok[:, at : at + NX * per], back[...])
        for x in range(NX):
            by_x[x, y, :, :width] = both[x * per : (x + 1) * per, width:]
            by_x[x, y, :, width:] = both[x * per : (x + 1) * per, :cut]
        stage[y, :, : width - cut] = both[:, cut:width]
        stage[y, :, width - cut :] = term(grad[:, at : at + NX * per], hid[...])
        stores.append(pltpu.make_async_copy(stage.at[y], by_y.at[y], out_sem.at[y]))
        stores[y].start()
    for store in stores:
        store.wait()
    keep.wait()


def add_x(got, out):
    acc = got[0].astype(jnp.float32)
    for i in range(1, NX):
        acc = acc + got[i].astype(jnp.float32)
    out[...] = acc.astype(jnp.bfloat16)


def turn(pos, part, *outs):
    for k, out in enumerate(outs):
        out[...] = part[(pos[1] + k) % NX]


def finish(from_y, *refs):
    parts, (gate, up, down) = refs[:NX], refs[NX:]
    acc = from_y[0].astype(jnp.float32)
    for i in range(1, NY):
        acc = acc + from_y[i].astype(jnp.float32)
    bcc = parts[0][...].astype(jnp.float32)
    for part in parts[1:]:
        bcc = bcc + part[...].astype(jnp.float32)
    width = up.shape[1]
    cut = acc.shape[1] - width
    up[...] = acc[:, :width]
    gate[:, :cut] = acc[:, width:]
    gate[:, cut:] = bcc[:, : width - cut]
    down[...] = bcc[:, width - cut :]


def a2a(value, axis):
    return lax.all_to_all(value, axis, split_axis=0, concat_axis=0, tiled=True)


def swap(value):
    return lax.ppermute(value, "c", [(0, 1), (1, 0)])


def along_z(value, by):
    return lax.ppermute(value, "z", [(i, (i + by) % NZ) for i in range(NZ)])


def step(
    tokens, out_grad, counts, block_moves, segment_ids, gate_weight, up_weight, down_weight
):
    bf = jnp.bfloat16
    f32 = jnp.float32
    slots, feat = tokens.shape
    per, hid = gate_weight.shape
    span = WORK * BLOCK
    model = 2 * NZ * feat
    weights = lax.all_gather(
        jnp.concatenate([gate_weight, up_weight, down_weight], axis=1), ROW, axis=0, tiled=True
    )
    pos = jnp.stack([lax.axis_index("y"), lax.axis_index("x"), counts[0], lax.axis_index("c"), lax.axis_index("z")])
    moves = block_moves.T
    box, work = pl.pallas_call(
        pack_x,
        out_shape=(
            jax.ShapeDtypeStruct((NX, 4 * BLOCK + NTAG, feat), bf),
            jax.ShapeDtypeStruct((2 * span, feat), bf),
        ),
        in_specs=[smem(), smem(), vmem(), vmem(), vmem()],
        out_specs=(vmem(), vmem()),
        scratch_shapes=[pltpu.VMEM((slots, feat), bf)],
        compiler_params=params(8),
        name="pack_x",
    )(pos, moves, segment_ids.reshape(CAP, BLOCK), tokens, out_grad)
    up2, down2 = along_z(work, 2), along_z(work, -2)
    up1, down1 = along_z(work, 1), along_z(work, -1)
    up3, down3, up4 = along_z(up2, 1), along_z(down2, -1), along_z(up2, 2)
    got = a2a(box, "x")
    box = pl.pallas_call(
        pack_y,
        out_shape=jax.ShapeDtypeStruct((NY, 2 * BLOCK + NTAG, feat), bf),
        in_specs=[smem(), smem(), vmem()],
        out_specs=vmem(),
        scratch_shapes=[pltpu.SMEM((NX,), jnp.int32)],
        compiler_params=params(8),
        name="pack_y",
    )(pos, moves, got)
    got = a2a(box, "y")
    box, total = pl.pallas_call(
        pick_arrival,
        out_shape=(
            jax.ShapeDtypeStruct((NZ, 2 * BLOCK, feat), bf),
            jax.ShapeDtypeStruct((8, BLOCK), f32),
        ),
        in_specs=[smem(), smem(), vmem()],
        out_specs=(vmem(), vmem()),
        compiler_params=params(8),
        name="pick_arrival",
    )(pos, moves, got)
    late = a2a(box, "z")
    pieces = (work, up1, up2, up3, up4, down3, down2, down1)
    mine = pl.pallas_call(
        gather_up,
        out_shape=jax.ShapeDtypeStruct((NZ, 2 * span, feat), bf),
        in_specs=[vmem()] * NZ,
        out_specs=vmem(),
        compiler_params=params(12),
        name="gather_up",
    )(*pieces)
    other = swap(mine)
    hbm = pl.BlockSpec(memory_space=pltpu.HBM)
    tok, grad = pl.pallas_call(
        lay_out,
        out_shape=(pltpu.HBM((span, model), bf), pltpu.HBM((span, model), bf)),
        in_specs=[smem(), smem(), vmem(), vmem(), vmem(), vmem()],
        out_specs=(hbm, hbm),
        scratch_shapes=[
            pltpu.VMEM((span, model), bf),
            pltpu.VMEM((span, model), bf),
            pltpu.SemaphoreType.DMA((2, NZ)),
        ],
        compiler_params=params(14),
        name="lay_out",
    )(pos, moves, mine, other, late, swap(late))

    wide_x, wide_y = hid + CUT, 2 * hid - CUT
    hidden, by_x, by_y = pl.pallas_call(
        compute,
        out_shape=(
            pltpu.HBM((span, hid), bf),
            pltpu.VMEM((NX, NY, per, wide_x), bf),
            pltpu.HBM((NY, NX * per, wide_y), bf),
        ),
        in_specs=[vmem(), hbm, hbm, hbm],
        out_specs=(hbm, vmem(), hbm),
        scratch_shapes=[
            pltpu.VMEM((span, model), bf),
            pltpu.VMEM((span, model), bf),
            pltpu.VMEM((model, 3 * hid), bf),
            pltpu.VMEM((span, hid), bf),
            pltpu.VMEM((span, 2 * hid), bf),
            pltpu.VMEM((NY, NX * per, wide_y), bf),
            pltpu.SemaphoreType.DMA((4,)),
            pltpu.SemaphoreType.DMA((NY,)),
            pltpu.SemaphoreType.DMA(()),
        ],
        compiler_params=params(36),
        name="compute",
    )(
        total,
        pltpu.with_memory_space_constraint(tok, pltpu.HBM),
        pltpu.with_memory_space_constraint(grad, pltpu.HBM),
        pltpu.with_memory_space_constraint(weights, pltpu.HBM),
    )

    part_y = lax.psum_scatter(
        by_y.reshape(NY * NX * per, wide_y), "y", scatter_dimension=0, tiled=True
    )
    part_x = pl.pallas_call(
        add_x,
        out_shape=jax.ShapeDtypeStruct((NY, per, wide_x), bf),
        in_specs=[vmem()],
        out_specs=vmem(),
        compiler_params=params(8),
        name="add_x",
    )(a2a(by_x, "x"))
    from_y = a2a(part_x, "y")
    turned = pl.pallas_call(
        turn,
        out_shape=tuple(jax.ShapeDtypeStruct((per, wide_y), bf) for _ in range(NX)),
        in_specs=[smem(), vmem()],
        out_specs=(vmem(),) * NX,
        compiler_params=params(8),
        name="turn",
    )(pos, part_y.reshape(NX, per, wide_y))
    from_x = [turned[0]] + [
        lax.ppermute(turned[k], "x", [(i, (i + k) % NX) for i in range(NX)]) for k in range(1, NX)
    ]
    gate_grad, up_grad, down_grad = pl.pallas_call(
        finish,
        out_shape=tuple(jax.ShapeDtypeStruct((per, hid), f32) for _ in range(3)),
        in_specs=[vmem()] * (NX + 1),
        out_specs=(vmem(), vmem(), vmem()),
        compiler_params=params(8),
        name="finish",
    )(from_y, *from_x)
    return (hidden, gate_grad, up_grad, down_grad)


def solution(mesh):
    torus = Mesh(mesh.devices.reshape(NY, NX, NZ, 2), ("y", "x", "z", "c"))
    return jax.shard_map(
        step,
        mesh=torus,
        in_specs=(P(ROW, COL), P(ROW, COL), P(ROW), P(), P(ROW), P(ROW, COL), P(ROW, COL), P(ROW, COL)),
        out_specs=(P(ROW, COL), P(ROW, COL), P(ROW, COL), P(ROW, COL)),
        check_vma=False,
    )
```

```python
import jax
import jax.numpy as jnp
from jax import lax
from jax.experimental import pallas as pl
from jax.experimental.pallas import tpu as pltpu
from jax.sharding import Mesh
from jax.sharding import PartitionSpec as P


BLOCK = 128
WORK = 4
CAP = 6
NY, NX, NZ = 8, 4, 8
ROW = ("y", "x")
COL = ("z", "c")
NTAG = 16
CUT = 256


def vmem():
    return pl.BlockSpec(memory_space=pltpu.VMEM)


def smem():
    return pl.BlockSpec(memory_space=pltpu.SMEM)


def params(mib, **kw):
    return pltpu.CompilerParams(vmem_limit_bytes=mib * 1024 * 1024, **kw)


def move_count(moves):
    return moves.shape[1]


def stack_x(pos, *refs):
    pieces, out, sems = refs[:NX], refs[NX], refs[NX + 1]
    sends = [
        pltpu.make_async_copy(piece, out.at[(pos[1] - k + NX) % NX], sems.at[k])
        for k, piece in enumerate(pieces)
    ]
    for send in sends:
        send.start()
    for send in sends:
        send.wait()


def pack_x(pos, moves, seg, tok, grad, box, work, masked):
    me = pos[0] * NX + pos[1]
    count = pos[2]
    span = WORK * BLOCK
    ids = seg[...]
    lane = lax.broadcasted_iota(jnp.int32, (CAP, BLOCK), 1)
    row = lax.broadcasted_iota(jnp.int32, (CAP, BLOCK), 0)
    ahead = jnp.concatenate([ids[1:], ids[-1:]], axis=0)
    joined = jnp.concatenate([ids[:, 1:], ahead[:, :1]], axis=1)
    mask = ((row * BLOCK + lane + 1 < count) & (joined == ids)).astype(jnp.float32)
    for b in range(CAP):
        rows = slice(b * BLOCK, (b + 1) * BLOCK)
        wide = jnp.broadcast_to(mask[b : b + 1, :], (BLOCK, BLOCK)).T
        masked[rows, :] = (grad[rows, :].astype(jnp.float32) * wide).astype(jnp.bfloat16)
    tally = jnp.sum(mask, axis=0, keepdims=True)
    for d in range(NX):
        box[d, 4 * BLOCK :, :] = jnp.broadcast_to(tally, (NTAG, BLOCK)).astype(jnp.bfloat16)

    def body(m, seen):
        src, dst, blk = moves[0, m], moves[1, m], moves[2, m]
        mine = src == me

        @pl.when(mine)
        def _():
            peer = dst % NX
            at = pl.multiple_of(seen * (2 * BLOCK), BLOCK)
            start = pl.multiple_of(blk * BLOCK, BLOCK)
            box[peer, pl.ds(at, BLOCK), :] = tok[pl.ds(start, BLOCK), :]
            box[peer, pl.ds(at + BLOCK, BLOCK), :] = masked[pl.ds(start, BLOCK), :]

        return jnp.where(mine, jnp.minimum(seen + 1, 1), seen)

    lax.fori_loop(0, move_count(moves), body, 0)
    work[...] = jnp.zeros_like(work)

    def own(b, nth):
        def gone(m, hit):
            return hit | ((moves[0, m] == me) & (moves[2, m] == b)).astype(jnp.int32)

        left = lax.fori_loop(0, move_count(moves), gone, 0)
        keep = (b * BLOCK < count) & (left == 0)

        @pl.when(keep & (nth < WORK))
        def _():
            start = pl.multiple_of(b * BLOCK, BLOCK)
            at = pl.multiple_of(nth * BLOCK, BLOCK)
            work[pl.ds(at, BLOCK), :] = tok[pl.ds(start, BLOCK), :]
            work[pl.ds(at + span, BLOCK), :] = masked[pl.ds(start, BLOCK), :]

        return nth + keep.astype(jnp.int32)

    lax.fori_loop(0, CAP, own, 0)


def pack_y(pos, moves, got, box, seen):
    my, mx = pos[0], pos[1]
    for i in range(NX):
        seen[i] = 0
    tally = got[0, 4 * BLOCK :, :].astype(jnp.float32)
    for i in range(1, NX):
        tally = tally + got[i, 4 * BLOCK :, :].astype(jnp.float32)
    for d in range(NY):
        box[d, 2 * BLOCK :, :] = tally.astype(jnp.bfloat16)

    def body(m, carry):
        src, dst = moves[0, m], moves[1, m]

        @pl.when(src // NX == my)
        def _():
            sx = src % NX
            nth = seen[sx]
            seen[sx] = jnp.minimum(nth + 1, 1)

            @pl.when(dst % NX == mx)
            def _():
                at = pl.multiple_of(nth * (2 * BLOCK), BLOCK)
                box[dst // NX, : 2 * BLOCK, :] = got[sx, pl.ds(at, 2 * BLOCK), :]

        return carry

    lax.fori_loop(0, move_count(moves), body, 0)


def pick_arrival(pos, moves, got, box, total):
    me = pos[0] * NX + pos[1]
    tally = got[0, 2 * BLOCK : 2 * BLOCK + 8, :].astype(jnp.float32)
    for i in range(1, NY):
        tally = tally + got[i, 2 * BLOCK : 2 * BLOCK + 8, :].astype(jnp.float32)
    total[...] = jnp.broadcast_to(jnp.sum(tally, axis=1, keepdims=True), total.shape)

    def came(m, at):
        return jnp.where(moves[1, m] == me, moves[0, m] // NX, at)

    sy = lax.fori_loop(0, move_count(moves), came, 0)
    for d in range(NZ):
        box[d] = got[sy, : 2 * BLOCK, :]


def gather_up(*refs):
    out = refs[-1]
    for k, piece in enumerate(refs[:-1]):
        out[k] = piece[...]


def lay_out(pos, moves, mine, other, late, late_other, tok_out, grad_out, tok, grad, sems):
    me = pos[0] * NX + pos[1]
    first = pos[3] == 0
    my_z = pos[4]
    span = WORK * BLOCK

    def own(b, nth):
        def gone(m, hit):
            return hit | ((moves[0, m] == me) & (moves[2, m] == b)).astype(jnp.int32)

        left = lax.fori_loop(0, move_count(moves), gone, 0)
        return nth + ((b * BLOCK < pos[2]) & (left == 0)).astype(jnp.int32)

    def came(m, hit):
        return hit | (moves[1, m] == me).astype(jnp.int32)

    nth = lax.fori_loop(0, CAP, own, 0)
    here = lax.fori_loop(0, move_count(moves), came, 0)
    there = (here == 1) & (nth < WORK)
    rows = pl.ds(pl.multiple_of(jnp.minimum(nth, WORK - 1) * BLOCK, BLOCK), BLOCK)
    sends = []
    for z in range(NZ):
        away = (my_z - z + NZ) % NZ
        for side in range(2):
            cols = slice((2 * z + side) * BLOCK, (2 * z + side + 1) * BLOCK)
            take = first if side == 0 else jnp.logical_not(first)
            block = jnp.where(take, mine[away], other[away])
            tok[:, cols] = block[:span]
            grad[:, cols] = block[span:]

            @pl.when(there)
            def _():
                extra = jnp.where(take, late[z], late_other[z])
                tok[rows, cols] = extra[:BLOCK]
                grad[rows, cols] = extra[BLOCK:]

        both = slice(2 * z * BLOCK, 2 * (z + 1) * BLOCK)
        for k, (ref, out) in enumerate(((tok, tok_out), (grad, grad_out))):
            sends.append(pltpu.make_async_copy(ref.at[:, both], out.at[:, both], sems.at[k, z]))
            sends[-1].start()
    for send in sends:
        send.wait()


def compute(
    total, tok_in, grad_in, weights, hidden, by_x, by_y,
    tok, grad, held, hid, back, stage, in_sem, out_sem, hid_sem,
):
    width = hid.shape[1]
    tile = width // 2
    per = by_x.shape[2]
    cut = by_x.shape[3] - width
    fore = 2 * width
    loads = (
        pltpu.make_async_copy(tok_in, tok, in_sem.at[0]),
        pltpu.make_async_copy(weights.at[:, :fore], held.at[:, :fore], in_sem.at[1]),
        pltpu.make_async_copy(grad_in, grad, in_sem.at[2]),
        pltpu.make_async_copy(weights.at[:, fore:], held.at[:, fore:], in_sem.at[3]),
    )
    for load in loads:
        load.start()
    loads[0].wait()
    loads[1].wait()
    sums = jnp.dot(tok[...], held[:, :fore], preferred_element_type=jnp.float32)
    loads[2].wait()
    loads[3].wait()
    for at in range(0, width, tile):
        gate_sum = sums[:, at : at + tile]
        up_sum = sums[:, width + at : width + at + tile]
        down_w = held[:, fore + at : fore + at + tile]
        back_sum = jnp.dot(grad[...], down_w, preferred_element_type=jnp.float32)
        logistic = jax.nn.sigmoid(gate_sum)
        act = gate_sum * logistic
        hid[:, at : at + tile] = (act * up_sum).astype(jnp.bfloat16)
        back[:, at : at + tile] = (
            back_sum * up_sum * logistic * (1.0 + gate_sum * (1.0 - logistic))
        ).astype(jnp.bfloat16)
        back[:, width + at : width + at + tile] = (back_sum * act).astype(jnp.bfloat16)
    keep = pltpu.make_async_copy(hid, hidden, hid_sem)
    keep.start()
    inv = 1.0 / total[0, 0]

    def term(left, right):
        out = lax.dot_general(
            left, right, (((0,), (0,)), ((), ())), preferred_element_type=jnp.float32
        )
        return (out * inv).astype(jnp.bfloat16)

    stores = []
    for y in range(NY):
        at = y * NX * per
        both = term(tok[:, at : at + NX * per], back[...])
        for x in range(NX):
            by_x[x, y, :, :width] = both[x * per : (x + 1) * per, width:]
            by_x[x, y, :, width:] = both[x * per : (x + 1) * per, :cut]
        stage[y, :, : width - cut] = both[:, cut:width]
        stage[y, :, width - cut :] = term(grad[:, at : at + NX * per], hid[...])
        stores.append(pltpu.make_async_copy(stage.at[y], by_y.at[y], out_sem.at[y]))
        stores[y].start()
    for store in stores:
        store.wait()
    keep.wait()


def add_x(got, out):
    acc = got[0].astype(jnp.float32)
    for i in range(1, NX):
        acc = acc + got[i].astype(jnp.float32)
    out[...] = acc.astype(jnp.bfloat16)


def turn(pos, part, *outs):
    for k, out in enumerate(outs):
        out[...] = part[(pos[1] + k) % NX]


def finish(from_y, *refs):
    parts, (gate, up, down) = refs[:NX], refs[NX:]
    acc = from_y[0].astype(jnp.float32)
    for i in range(1, NY):
        acc = acc + from_y[i].astype(jnp.float32)
    bcc = parts[0][...].astype(jnp.float32)
    for part in parts[1:]:
        bcc = bcc + part[...].astype(jnp.float32)
    width = up.shape[1]
    cut = acc.shape[1] - width
    up[...] = acc[:, :width]
    gate[:, :cut] = acc[:, width:]
    gate[:, cut:] = bcc[:, : width - cut]
    down[...] = bcc[:, width - cut :]


def a2a(value, axis):
    return lax.all_to_all(value, axis, split_axis=0, concat_axis=0, tiled=True)


def swap(value):
    return lax.ppermute(value, "c", [(0, 1), (1, 0)])


def along_x(value, by):
    return lax.ppermute(value, "x", [(i, (i + by) % NX) for i in range(NX)])


def along_z(value, by):
    return lax.ppermute(value, "z", [(i, (i + by) % NZ) for i in range(NZ)])


def step(
    tokens, out_grad, counts, block_moves, segment_ids, gate_weight, up_weight, down_weight
):
    bf = jnp.bfloat16
    f32 = jnp.float32
    slots, feat = tokens.shape
    per, hid = gate_weight.shape
    span = WORK * BLOCK
    model = 2 * NZ * feat
    hbm = pl.BlockSpec(memory_space=pltpu.HBM)
    pos = jnp.stack([lax.axis_index("y"), lax.axis_index("x"), counts[0], lax.axis_index("c"), lax.axis_index("z")])
    moves = block_moves.T
    joined = jnp.concatenate([gate_weight, up_weight, down_weight], axis=1)
    shifted = [along_x(joined, k) for k in range(1, NX)]
    stacked = pl.pallas_call(
        stack_x,
        out_shape=pltpu.HBM((NX, per, 3 * hid), bf),
        in_specs=[smem()] + [pl.BlockSpec(memory_space=pl.ANY)] * NX,
        out_specs=hbm,
        scratch_shapes=[pltpu.SemaphoreType.DMA((NX,))],
        compiler_params=params(8),
        name="stack_x",
    )(pos, joined, *shifted)
    weights = lax.all_gather(stacked.reshape(NX * per, 3 * hid), "y", axis=0, tiled=True)
    box, work = pl.pallas_call(
        pack_x,
        out_shape=(
            jax.ShapeDtypeStruct((NX, 4 * BLOCK + NTAG, feat), bf),
            jax.ShapeDtypeStruct((2 * span, feat), bf),
        ),
        in_specs=[smem(), smem(), vmem(), vmem(), vmem()],
        out_specs=(vmem(), vmem()),
        scratch_shapes=[pltpu.VMEM((slots, feat), bf)],
        compiler_params=params(8),
        name="pack_x",
    )(pos, moves, segment_ids.reshape(CAP, BLOCK), tokens, out_grad)
    up2, down2 = along_z(work, 2), along_z(work, -2)
    up1, down1 = along_z(work, 1), along_z(work, -1)
    up3, down3, up4 = along_z(up2, 1), along_z(down2, -1), along_z(up2, 2)
    got = a2a(box, "x")
    box = pl.pallas_call(
        pack_y,
        out_shape=jax.ShapeDtypeStruct((NY, 2 * BLOCK + NTAG, feat), bf),
        in_specs=[smem(), smem(), vmem()],
        out_specs=vmem(),
        scratch_shapes=[pltpu.SMEM((NX,), jnp.int32)],
        compiler_params=params(8),
        name="pack_y",
    )(pos, moves, got)
    got = a2a(box, "y")
    box, total = pl.pallas_call(
        pick_arrival,
        out_shape=(
            jax.ShapeDtypeStruct((NZ, 2 * BLOCK, feat), bf),
            jax.ShapeDtypeStruct((8, BLOCK), f32),
        ),
        in_specs=[smem(), smem(), vmem()],
        out_specs=(vmem(), vmem()),
        compiler_params=params(8),
        name="pick_arrival",
    )(pos, moves, got)
    late = a2a(box, "z")
    pieces = (work, up1, up2, up3, up4, down3, down2, down1)
    mine = pl.pallas_call(
        gather_up,
        out_shape=jax.ShapeDtypeStruct((NZ, 2 * span, feat), bf),
        in_specs=[vmem()] * NZ,
        out_specs=vmem(),
        compiler_params=params(12),
        name="gather_up",
    )(*pieces)
    other = swap(mine)
    tok, grad = pl.pallas_call(
        lay_out,
        out_shape=(pltpu.HBM((span, model), bf), pltpu.HBM((span, model), bf)),
        in_specs=[smem(), smem(), vmem(), vmem(), vmem(), vmem()],
        out_specs=(hbm, hbm),
        scratch_shapes=[
            pltpu.VMEM((span, model), bf),
            pltpu.VMEM((span, model), bf),
            pltpu.SemaphoreType.DMA((2, NZ)),
        ],
        compiler_params=params(14),
        name="lay_out",
    )(pos, moves, mine, other, late, swap(late))

    wide_x, wide_y = hid + CUT, 2 * hid - CUT
    hidden, by_x, by_y = pl.pallas_call(
        compute,
        out_shape=(
            pltpu.HBM((span, hid), bf),
            pltpu.VMEM((NX, NY, per, wide_x), bf),
            pltpu.HBM((NY, NX * per, wide_y), bf),
        ),
        in_specs=[vmem(), hbm, hbm, hbm],
        out_specs=(hbm, vmem(), hbm),
        scratch_shapes=[
            pltpu.VMEM((span, model), bf),
            pltpu.VMEM((span, model), bf),
            pltpu.VMEM((model, 3 * hid), bf),
            pltpu.VMEM((span, hid), bf),
            pltpu.VMEM((span, 2 * hid), bf),
            pltpu.VMEM((NY, NX * per, wide_y), bf),
            pltpu.SemaphoreType.DMA((4,)),
            pltpu.SemaphoreType.DMA((NY,)),
            pltpu.SemaphoreType.DMA(()),
        ],
        compiler_params=params(36),
        name="compute",
    )(
        total,
        pltpu.with_memory_space_constraint(tok, pltpu.HBM),
        pltpu.with_memory_space_constraint(grad, pltpu.HBM),
        pltpu.with_memory_space_constraint(weights, pltpu.HBM),
    )

    part_y = lax.psum_scatter(
        by_y.reshape(NY * NX * per, wide_y), "y", scatter_dimension=0, tiled=True
    )
    part_x = pl.pallas_call(
        add_x,
        out_shape=jax.ShapeDtypeStruct((NY, per, wide_x), bf),
        in_specs=[vmem()],
        out_specs=vmem(),
        compiler_params=params(8),
        name="add_x",
    )(a2a(by_x, "x"))
    from_y = a2a(part_x, "y")
    turned = pl.pallas_call(
        turn,
        out_shape=tuple(jax.ShapeDtypeStruct((per, wide_y), bf) for _ in range(NX)),
        in_specs=[smem(), vmem()],
        out_specs=(vmem(),) * NX,
        compiler_params=params(8),
        name="turn",
    )(pos, part_y.reshape(NX, per, wide_y))
    from_x = [turned[0]] + [
        along_x(turned[k], k) for k in range(1, NX)
    ]
    gate_grad, up_grad, down_grad = pl.pallas_call(
        finish,
        out_shape=tuple(jax.ShapeDtypeStruct((per, hid), f32) for _ in range(3)),
        in_specs=[vmem()] * (NX + 1),
        out_specs=(vmem(), vmem(), vmem()),
        compiler_params=params(8),
        name="finish",
    )(from_y, *from_x)
    return (hidden, gate_grad, up_grad, down_grad)


def solution(mesh):
    torus = Mesh(mesh.devices.reshape(NY, NX, NZ, 2), ("y", "x", "z", "c"))
    return jax.shard_map(
        step,
        mesh=torus,
        in_specs=(P(ROW, COL), P(ROW, COL), P(ROW), P(), P(ROW), P(ROW, COL), P(ROW, COL), P(ROW, COL)),
        out_specs=(P(ROW, COL), P(ROW, COL), P(ROW, COL), P(ROW, COL)),
        check_vma=False,
    )
```

```python
import jax
import jax.numpy as jnp
from jax import lax
from jax.experimental import pallas as pl
from jax.experimental.pallas import tpu as pltpu
from jax.sharding import Mesh
from jax.sharding import PartitionSpec as P


BLOCK = 128
WORK = 4
CAP = 6
NY, NX, NZ = 8, 4, 8
ROW = ("y", "x")
COL = ("z", "c")
NTAG = 16
CUT = 256


def vmem():
    return pl.BlockSpec(memory_space=pltpu.VMEM)


def smem():
    return pl.BlockSpec(memory_space=pltpu.SMEM)


def params(mib, **kw):
    return pltpu.CompilerParams(vmem_limit_bytes=mib * 1024 * 1024, **kw)


def move_count(moves):
    return moves.shape[1]


def pack_x(pos, moves, seg, tok, grad, box, work, masked):
    me = pos[0] * NX + pos[1]
    count = pos[2]
    span = WORK * BLOCK
    ids = seg[...]
    lane = lax.broadcasted_iota(jnp.int32, (CAP, BLOCK), 1)
    row = lax.broadcasted_iota(jnp.int32, (CAP, BLOCK), 0)
    ahead = jnp.concatenate([ids[1:], ids[-1:]], axis=0)
    joined = jnp.concatenate([ids[:, 1:], ahead[:, :1]], axis=1)
    mask = ((row * BLOCK + lane + 1 < count) & (joined == ids)).astype(jnp.float32)
    for b in range(CAP):
        rows = slice(b * BLOCK, (b + 1) * BLOCK)
        wide = jnp.broadcast_to(mask[b : b + 1, :], (BLOCK, BLOCK)).T
        masked[rows, :] = (grad[rows, :].astype(jnp.float32) * wide).astype(jnp.bfloat16)
    tally = jnp.sum(mask, axis=0, keepdims=True)
    for d in range(NX):
        box[d, 4 * BLOCK :, :] = jnp.broadcast_to(tally, (NTAG, BLOCK)).astype(jnp.bfloat16)

    def body(m, seen):
        src, dst, blk = moves[0, m], moves[1, m], moves[2, m]
        mine = src == me

        @pl.when(mine)
        def _():
            peer = dst % NX
            at = pl.multiple_of(seen * (2 * BLOCK), BLOCK)
            start = pl.multiple_of(blk * BLOCK, BLOCK)
            box[peer, pl.ds(at, BLOCK), :] = tok[pl.ds(start, BLOCK), :]
            box[peer, pl.ds(at + BLOCK, BLOCK), :] = masked[pl.ds(start, BLOCK), :]

        return jnp.where(mine, jnp.minimum(seen + 1, 1), seen)

    lax.fori_loop(0, move_count(moves), body, 0)
    work[...] = jnp.zeros_like(work)

    def own(b, nth):
        def gone(m, hit):
            return hit | ((moves[0, m] == me) & (moves[2, m] == b)).astype(jnp.int32)

        left = lax.fori_loop(0, move_count(moves), gone, 0)
        keep = (b * BLOCK < count) & (left == 0)

        @pl.when(keep & (nth < WORK))
        def _():
            start = pl.multiple_of(b * BLOCK, BLOCK)
            at = pl.multiple_of(nth * BLOCK, BLOCK)
            work[pl.ds(at, BLOCK), :] = tok[pl.ds(start, BLOCK), :]
            work[pl.ds(at + span, BLOCK), :] = masked[pl.ds(start, BLOCK), :]

        return nth + keep.astype(jnp.int32)

    lax.fori_loop(0, CAP, own, 0)


def pack_y(pos, moves, got, box, seen):
    my, mx = pos[0], pos[1]
    for i in range(NX):
        seen[i] = 0
    tally = got[0, 4 * BLOCK :, :].astype(jnp.float32)
    for i in range(1, NX):
        tally = tally + got[i, 4 * BLOCK :, :].astype(jnp.float32)
    for d in range(NY):
        box[d, 2 * BLOCK :, :] = tally.astype(jnp.bfloat16)

    def body(m, carry):
        src, dst = moves[0, m], moves[1, m]

        @pl.when(src // NX == my)
        def _():
            sx = src % NX
            nth = seen[sx]
            seen[sx] = jnp.minimum(nth + 1, 1)

            @pl.when(dst % NX == mx)
            def _():
                at = pl.multiple_of(nth * (2 * BLOCK), BLOCK)
                box[dst // NX, : 2 * BLOCK, :] = got[sx, pl.ds(at, 2 * BLOCK), :]

        return carry

    lax.fori_loop(0, move_count(moves), body, 0)


def pick_arrival(pos, moves, got, box, total):
    me = pos[0] * NX + pos[1]
    tally = got[0, 2 * BLOCK : 2 * BLOCK + 8, :].astype(jnp.float32)
    for i in range(1, NY):
        tally = tally + got[i, 2 * BLOCK : 2 * BLOCK + 8, :].astype(jnp.float32)
    total[...] = jnp.broadcast_to(jnp.sum(tally, axis=1, keepdims=True), total.shape)

    def came(m, at):
        return jnp.where(moves[1, m] == me, moves[0, m] // NX, at)

    sy = lax.fori_loop(0, move_count(moves), came, 0)
    for d in range(NZ):
        box[d] = got[sy, : 2 * BLOCK, :]


def gather_up(*refs):
    out = refs[-1]
    for k, piece in enumerate(refs[:-1]):
        out[k] = piece[...]


def lay_out(pos, moves, mine, other, late, late_other, tok_out, grad_out, tok, grad, sems):
    me = pos[0] * NX + pos[1]
    first = pos[3] == 0
    my_z = pos[4]
    span = WORK * BLOCK

    def own(b, nth):
        def gone(m, hit):
            return hit | ((moves[0, m] == me) & (moves[2, m] == b)).astype(jnp.int32)

        left = lax.fori_loop(0, move_count(moves), gone, 0)
        return nth + ((b * BLOCK < pos[2]) & (left == 0)).astype(jnp.int32)

    def came(m, hit):
        return hit | (moves[1, m] == me).astype(jnp.int32)

    nth = lax.fori_loop(0, CAP, own, 0)
    here = lax.fori_loop(0, move_count(moves), came, 0)
    there = (here == 1) & (nth < WORK)
    rows = pl.ds(pl.multiple_of(jnp.minimum(nth, WORK - 1) * BLOCK, BLOCK), BLOCK)
    sends = []
    for z in range(NZ):
        away = (my_z - z + NZ) % NZ
        for side in range(2):
            cols = slice((2 * z + side) * BLOCK, (2 * z + side + 1) * BLOCK)
            take = first if side == 0 else jnp.logical_not(first)
            block = jnp.where(take, mine[away], other[away])
            tok[:, cols] = block[:span]
            grad[:, cols] = block[span:]

            @pl.when(there)
            def _():
                extra = jnp.where(take, late[z], late_other[z])
                tok[rows, cols] = extra[:BLOCK]
                grad[rows, cols] = extra[BLOCK:]

        both = slice(2 * z * BLOCK, 2 * (z + 1) * BLOCK)
        for k, (ref, out) in enumerate(((tok, tok_out), (grad, grad_out))):
            sends.append(pltpu.make_async_copy(ref.at[:, both], out.at[:, both], sems.at[k, z]))
            sends[-1].start()
    for send in sends:
        send.wait()


def compute(
    total, tok_in, grad_in, weights, hidden, by_x, by_y,
    tok, grad, held, hid, back, stage, in_sem, out_sem, hid_sem,
):
    width = hid.shape[1]
    tile = width // 2
    per = by_x.shape[2]
    cut = by_x.shape[3] - width
    thirds = [slice(k * width, (k + 1) * width) for k in range(3)]
    take_tok = pltpu.make_async_copy(tok_in, tok, in_sem.at[3])
    take_grad = pltpu.make_async_copy(grad_in, grad, in_sem.at[4])
    take = [
        pltpu.make_async_copy(weights.at[:, cols], held.at[:, cols], in_sem.at[k])
        for k, cols in enumerate(thirds)
    ]
    for load in (take_tok, take[0], take[1], take_grad, take[2]):
        load.start()
    take_tok.wait()
    take[0].wait()
    gate_all = jnp.dot(tok[...], held[:, thirds[0]], preferred_element_type=jnp.float32)
    take[1].wait()
    up_all = jnp.dot(tok[...], held[:, thirds[1]], preferred_element_type=jnp.float32)
    take_grad.wait()
    take[2].wait()
    for at in range(0, width, tile):
        gate_sum = gate_all[:, at : at + tile]
        up_sum = up_all[:, at : at + tile]
        down_w = held[:, 2 * width + at : 2 * width + at + tile]
        back_sum = jnp.dot(grad[...], down_w, preferred_element_type=jnp.float32)
        logistic = jax.nn.sigmoid(gate_sum)
        act = gate_sum * logistic
        hid[:, at : at + tile] = (act * up_sum).astype(jnp.bfloat16)
        back[:, at : at + tile] = (
            back_sum * up_sum * logistic * (1.0 + gate_sum * (1.0 - logistic))
        ).astype(jnp.bfloat16)
        back[:, width + at : width + at + tile] = (back_sum * act).astype(jnp.bfloat16)
    keep = pltpu.make_async_copy(hid, hidden, hid_sem)
    keep.start()
    inv = 1.0 / total[0, 0]

    def term(left, right):
        out = lax.dot_general(
            left, right, (((0,), (0,)), ((), ())), preferred_element_type=jnp.float32
        )
        return (out * inv).astype(jnp.bfloat16)

    stores = []
    for y in range(NY):
        rows = slice(y * NX * per, (y + 1) * NX * per)
        stage[y, :, : width - cut] = term(tok[:, rows], back[:, cut:width])
        stage[y, :, width - cut :] = term(grad[:, rows], hid[...])
        stores.append(pltpu.make_async_copy(stage.at[y], by_y.at[y], out_sem.at[y]))
        stores[y].start()
    for y in range(NY):
        rows = slice(y * NX * per, (y + 1) * NX * per)
        up = term(tok[:, rows], back[:, width:])
        gate = term(tok[:, rows], back[:, :cut])
        for x in range(NX):
            by_x[x, y, :, :width] = up[x * per : (x + 1) * per]
            by_x[x, y, :, width:] = gate[x * per : (x + 1) * per]
    for store in stores:
        store.wait()
    keep.wait()


def add_x(got, out):
    acc = got[0].astype(jnp.float32)
    for i in range(1, NX):
        acc = acc + got[i].astype(jnp.float32)
    out[...] = acc.astype(jnp.bfloat16)


def turn(pos, part, *outs):
    for k, out in enumerate(outs):
        out[...] = part[(pos[1] + k) % NX]


def finish(from_y, *refs):
    parts, (gate, up, down) = refs[:NX], refs[NX:]
    acc = from_y[0].astype(jnp.float32)
    for i in range(1, NY):
        acc = acc + from_y[i].astype(jnp.float32)
    bcc = parts[0][...].astype(jnp.float32)
    for part in parts[1:]:
        bcc = bcc + part[...].astype(jnp.float32)
    width = up.shape[1]
    cut = acc.shape[1] - width
    up[...] = acc[:, :width]
    gate[:, :cut] = acc[:, width:]
    gate[:, cut:] = bcc[:, : width - cut]
    down[...] = bcc[:, width - cut :]


def a2a(value, axis):
    return lax.all_to_all(value, axis, split_axis=0, concat_axis=0, tiled=True)


def swap(value):
    return lax.ppermute(value, "c", [(0, 1), (1, 0)])


def along_z(value, by):
    return lax.ppermute(value, "z", [(i, (i + by) % NZ) for i in range(NZ)])


def step(
    tokens, out_grad, counts, block_moves, segment_ids, gate_weight, up_weight, down_weight
):
    bf = jnp.bfloat16
    f32 = jnp.float32
    slots, feat = tokens.shape
    per, hid = gate_weight.shape
    span = WORK * BLOCK
    model = 2 * NZ * feat
    weights = lax.all_gather(
        jnp.concatenate([gate_weight, up_weight, down_weight], axis=1), ROW, axis=0, tiled=True
    )
    pos = jnp.stack([lax.axis_index("y"), lax.axis_index("x"), counts[0], lax.axis_index("c"), lax.axis_index("z")])
    moves = block_moves.T
    box, work = pl.pallas_call(
        pack_x,
        out_shape=(
            jax.ShapeDtypeStruct((NX, 4 * BLOCK + NTAG, feat), bf),
            jax.ShapeDtypeStruct((2 * span, feat), bf),
        ),
        in_specs=[smem(), smem(), vmem(), vmem(), vmem()],
        out_specs=(vmem(), vmem()),
        scratch_shapes=[pltpu.VMEM((slots, feat), bf)],
        compiler_params=params(8),
        name="pack_x",
    )(pos, moves, segment_ids.reshape(CAP, BLOCK), tokens, out_grad)
    up2, down2 = along_z(work, 2), along_z(work, -2)
    up1, down1 = along_z(work, 1), along_z(work, -1)
    up3, down3, up4 = along_z(up2, 1), along_z(down2, -1), along_z(up2, 2)
    got = a2a(box, "x")
    box = pl.pallas_call(
        pack_y,
        out_shape=jax.ShapeDtypeStruct((NY, 2 * BLOCK + NTAG, feat), bf),
        in_specs=[smem(), smem(), vmem()],
        out_specs=vmem(),
        scratch_shapes=[pltpu.SMEM((NX,), jnp.int32)],
        compiler_params=params(8),
        name="pack_y",
    )(pos, moves, got)
    got = a2a(box, "y")
    box, total = pl.pallas_call(
        pick_arrival,
        out_shape=(
            jax.ShapeDtypeStruct((NZ, 2 * BLOCK, feat), bf),
            jax.ShapeDtypeStruct((8, BLOCK), f32),
        ),
        in_specs=[smem(), smem(), vmem()],
        out_specs=(vmem(), vmem()),
        compiler_params=params(8),
        name="pick_arrival",
    )(pos, moves, got)
    late = a2a(box, "z")
    pieces = (work, up1, up2, up3, up4, down3, down2, down1)
    mine = pl.pallas_call(
        gather_up,
        out_shape=jax.ShapeDtypeStruct((NZ, 2 * span, feat), bf),
        in_specs=[vmem()] * NZ,
        out_specs=vmem(),
        compiler_params=params(12),
        name="gather_up",
    )(*pieces)
    other = swap(mine)
    hbm = pl.BlockSpec(memory_space=pltpu.HBM)
    tok, grad = pl.pallas_call(
        lay_out,
        out_shape=(pltpu.HBM((span, model), bf), pltpu.HBM((span, model), bf)),
        in_specs=[smem(), smem(), vmem(), vmem(), vmem(), vmem()],
        out_specs=(hbm, hbm),
        scratch_shapes=[
            pltpu.VMEM((span, model), bf),
            pltpu.VMEM((span, model), bf),
            pltpu.SemaphoreType.DMA((2, NZ)),
        ],
        compiler_params=params(14),
        name="lay_out",
    )(pos, moves, mine, other, late, swap(late))

    wide_x, wide_y = hid + CUT, 2 * hid - CUT
    hidden, by_x, by_y = pl.pallas_call(
        compute,
        out_shape=(
            pltpu.HBM((span, hid), bf),
            pltpu.VMEM((NX, NY, per, wide_x), bf),
            pltpu.HBM((NY, NX * per, wide_y), bf),
        ),
        in_specs=[vmem(), hbm, hbm, hbm],
        out_specs=(hbm, vmem(), hbm),
        scratch_shapes=[
            pltpu.VMEM((span, model), bf),
            pltpu.VMEM((span, model), bf),
            pltpu.VMEM((model, 3 * hid), bf),
            pltpu.VMEM((span, hid), bf),
            pltpu.VMEM((span, 2 * hid), bf),
            pltpu.VMEM((NY, NX * per, wide_y), bf),
            pltpu.SemaphoreType.DMA((5,)),
            pltpu.SemaphoreType.DMA((NY,)),
            pltpu.SemaphoreType.DMA(()),
        ],
        compiler_params=params(36),
        name="compute",
    )(
        total,
        pltpu.with_memory_space_constraint(tok, pltpu.HBM),
        pltpu.with_memory_space_constraint(grad, pltpu.HBM),
        pltpu.with_memory_space_constraint(weights, pltpu.HBM),
    )

    part_y = lax.psum_scatter(
        by_y.reshape(NY * NX * per, wide_y), "y", scatter_dimension=0, tiled=True
    )
    part_x = pl.pallas_call(
        add_x,
        out_shape=jax.ShapeDtypeStruct((NY, per, wide_x), bf),
        in_specs=[vmem()],
        out_specs=vmem(),
        compiler_params=params(8),
        name="add_x",
    )(a2a(by_x, "x"))
    from_y = a2a(part_x, "y")
    turned = pl.pallas_call(
        turn,
        out_shape=tuple(jax.ShapeDtypeStruct((per, wide_y), bf) for _ in range(NX)),
        in_specs=[smem(), vmem()],
        out_specs=(vmem(),) * NX,
        compiler_params=params(8),
        name="turn",
    )(pos, part_y.reshape(NX, per, wide_y))
    from_x = [turned[0]] + [
        lax.ppermute(turned[k], "x", [(i, (i + k) % NX) for i in range(NX)]) for k in range(1, NX)
    ]
    gate_grad, up_grad, down_grad = pl.pallas_call(
        finish,
        out_shape=tuple(jax.ShapeDtypeStruct((per, hid), f32) for _ in range(3)),
        in_specs=[vmem()] * (NX + 1),
        out_specs=(vmem(), vmem(), vmem()),
        compiler_params=params(8),
        name="finish",
    )(from_y, *from_x)
    return (hidden, gate_grad, up_grad, down_grad)


def solution(mesh):
    torus = Mesh(mesh.devices.reshape(NY, NX, NZ, 2), ("y", "x", "z", "c"))
    return jax.shard_map(
        step,
        mesh=torus,
        in_specs=(P(ROW, COL), P(ROW, COL), P(ROW), P(), P(ROW), P(ROW, COL), P(ROW, COL), P(ROW, COL)),
        out_specs=(P(ROW, COL), P(ROW, COL), P(ROW, COL), P(ROW, COL)),
        check_vma=False,
    )
```

```python
import jax
import jax.numpy as jnp
from jax import lax
from jax.experimental import pallas as pl
from jax.experimental.pallas import tpu as pltpu
from jax.sharding import Mesh
from jax.sharding import PartitionSpec as P


BLOCK = 128
WORK = 4
CAP = 6
NY, NX, NZ = 8, 4, 8
ROW = ("y", "x")
COL = ("z", "c")
NTAG = 16
CUT = 256


def vmem():
    return pl.BlockSpec(memory_space=pltpu.VMEM)


def smem():
    return pl.BlockSpec(memory_space=pltpu.SMEM)


def params(mib, **kw):
    return pltpu.CompilerParams(vmem_limit_bytes=mib * 1024 * 1024, **kw)


def move_count(moves):
    return moves.shape[1]


def pack_x(pos, moves, seg, tok, grad, box, work, masked):
    me = pos[0] * NX + pos[1]
    count = pos[2]
    span = WORK * BLOCK
    ids = seg[...]
    lane = lax.broadcasted_iota(jnp.int32, (CAP, BLOCK), 1)
    row = lax.broadcasted_iota(jnp.int32, (CAP, BLOCK), 0)
    ahead = jnp.concatenate([ids[1:], ids[-1:]], axis=0)
    joined = jnp.concatenate([ids[:, 1:], ahead[:, :1]], axis=1)
    mask = ((row * BLOCK + lane + 1 < count) & (joined == ids)).astype(jnp.float32)
    for b in range(CAP):
        rows = slice(b * BLOCK, (b + 1) * BLOCK)
        wide = jnp.broadcast_to(mask[b : b + 1, :], (BLOCK, BLOCK)).T
        masked[rows, :] = (grad[rows, :].astype(jnp.float32) * wide).astype(jnp.bfloat16)
    tally = jnp.sum(mask, axis=0, keepdims=True)
    for d in range(NX):
        box[d, 4 * BLOCK :, :] = jnp.broadcast_to(tally, (NTAG, BLOCK)).astype(jnp.bfloat16)

    def body(m, seen):
        src, dst, blk = moves[0, m], moves[1, m], moves[2, m]
        mine = src == me

        @pl.when(mine)
        def _():
            peer = dst % NX
            at = pl.multiple_of(seen * (2 * BLOCK), BLOCK)
            start = pl.multiple_of(blk * BLOCK, BLOCK)
            box[peer, pl.ds(at, BLOCK), :] = tok[pl.ds(start, BLOCK), :]
            box[peer, pl.ds(at + BLOCK, BLOCK), :] = masked[pl.ds(start, BLOCK), :]

        return jnp.where(mine, jnp.minimum(seen + 1, 1), seen)

    lax.fori_loop(0, move_count(moves), body, 0)
    work[...] = jnp.zeros_like(work)

    def own(b, nth):
        def gone(m, hit):
            return hit | ((moves[0, m] == me) & (moves[2, m] == b)).astype(jnp.int32)

        left = lax.fori_loop(0, move_count(moves), gone, 0)
        keep = (b * BLOCK < count) & (left == 0)

        @pl.when(keep & (nth < WORK))
        def _():
            start = pl.multiple_of(b * BLOCK, BLOCK)
            at = pl.multiple_of(nth * BLOCK, BLOCK)
            work[pl.ds(at, BLOCK), :] = tok[pl.ds(start, BLOCK), :]
            work[pl.ds(at + span, BLOCK), :] = masked[pl.ds(start, BLOCK), :]

        return nth + keep.astype(jnp.int32)

    lax.fori_loop(0, CAP, own, 0)


def pack_y(pos, moves, got, box, seen):
    my, mx = pos[0], pos[1]
    for i in range(NX):
        seen[i] = 0
    tally = got[0, 4 * BLOCK :, :].astype(jnp.float32)
    for i in range(1, NX):
        tally = tally + got[i, 4 * BLOCK :, :].astype(jnp.float32)
    for d in range(NY):
        box[d, 2 * BLOCK :, :] = tally.astype(jnp.bfloat16)

    def body(m, carry):
        src, dst = moves[0, m], moves[1, m]

        @pl.when(src // NX == my)
        def _():
            sx = src % NX
            nth = seen[sx]
            seen[sx] = jnp.minimum(nth + 1, 1)

            @pl.when(dst % NX == mx)
            def _():
                at = pl.multiple_of(nth * (2 * BLOCK), BLOCK)
                box[dst // NX, : 2 * BLOCK, :] = got[sx, pl.ds(at, 2 * BLOCK), :]

        return carry

    lax.fori_loop(0, move_count(moves), body, 0)


def pick_arrival(pos, moves, got, box, total):
    me = pos[0] * NX + pos[1]
    tally = got[0, 2 * BLOCK : 2 * BLOCK + 8, :].astype(jnp.float32)
    for i in range(1, NY):
        tally = tally + got[i, 2 * BLOCK : 2 * BLOCK + 8, :].astype(jnp.float32)
    total[...] = jnp.broadcast_to(jnp.sum(tally, axis=1, keepdims=True), total.shape)

    def came(m, at):
        return jnp.where(moves[1, m] == me, moves[0, m] // NX, at)

    sy = lax.fori_loop(0, move_count(moves), came, 0)
    for d in range(NZ):
        box[d] = got[sy, : 2 * BLOCK, :]


def gather_up(*refs):
    out = refs[-1]
    for k, piece in enumerate(refs[:-1]):
        out[k] = piece[...]


def lay_out(pos, moves, mine, other, late, late_other, tok_out, grad_out, tok, grad, sems):
    me = pos[0] * NX + pos[1]
    first = pos[3] == 0
    my_z = pos[4]
    span = WORK * BLOCK

    def own(b, nth):
        def gone(m, hit):
            return hit | ((moves[0, m] == me) & (moves[2, m] == b)).astype(jnp.int32)

        left = lax.fori_loop(0, move_count(moves), gone, 0)
        return nth + ((b * BLOCK < pos[2]) & (left == 0)).astype(jnp.int32)

    def came(m, hit):
        return hit | (moves[1, m] == me).astype(jnp.int32)

    nth = lax.fori_loop(0, CAP, own, 0)
    here = lax.fori_loop(0, move_count(moves), came, 0)
    there = (here == 1) & (nth < WORK)
    rows = pl.ds(pl.multiple_of(jnp.minimum(nth, WORK - 1) * BLOCK, BLOCK), BLOCK)
    sends = []
    for z in range(NZ):
        away = (my_z - z + NZ) % NZ
        for side in range(2):
            cols = slice((2 * z + side) * BLOCK, (2 * z + side + 1) * BLOCK)
            take = first if side == 0 else jnp.logical_not(first)
            block = jnp.where(take, mine[away], other[away])
            tok[:, cols] = block[:span]
            grad[:, cols] = block[span:]

            @pl.when(there)
            def _():
                extra = jnp.where(take, late[z], late_other[z])
                tok[rows, cols] = extra[:BLOCK]
                grad[rows, cols] = extra[BLOCK:]

        both = slice(2 * z * BLOCK, 2 * (z + 1) * BLOCK)
        for k, (ref, out) in enumerate(((tok, tok_out), (grad, grad_out))):
            sends.append(pltpu.make_async_copy(ref.at[:, both], out.at[:, both], sems.at[k, z]))
            sends[-1].start()
    for send in sends:
        send.wait()


def compute(
    total, tok_in, grad_in, weights, hidden, by_x, by_y,
    tok, grad, held, hid, back, stage, in_sem, out_sem, hid_sem,
):
    width = hid.shape[1]
    tile = width // 2
    per = by_x.shape[2]
    cut = by_x.shape[3] - width
    thirds = [slice(k * width, (k + 1) * width) for k in range(3)]
    take_tok = pltpu.make_async_copy(tok_in, tok, in_sem.at[3])
    take_grad = pltpu.make_async_copy(grad_in, grad, in_sem.at[4])
    take = [
        pltpu.make_async_copy(weights.at[:, cols], held.at[:, cols], in_sem.at[k])
        for k, cols in enumerate(thirds)
    ]
    for load in (take_tok, take[0], take[1], take_grad, take[2]):
        load.start()
    take_tok.wait()
    take[0].wait()
    gate_all = jnp.dot(tok[...], held[:, thirds[0]], preferred_element_type=jnp.float32)
    take[1].wait()
    up_all = jnp.dot(tok[...], held[:, thirds[1]], preferred_element_type=jnp.float32)
    take_grad.wait()
    take[2].wait()
    for at in range(0, width, tile):
        gate_sum = gate_all[:, at : at + tile]
        up_sum = up_all[:, at : at + tile]
        down_w = held[:, 2 * width + at : 2 * width + at + tile]
        back_sum = jnp.dot(grad[...], down_w, preferred_element_type=jnp.float32)
        logistic = jax.nn.sigmoid(gate_sum)
        act = gate_sum * logistic
        hid[:, at : at + tile] = (act * up_sum).astype(jnp.bfloat16)
        back[:, at : at + tile] = (
            back_sum * up_sum * logistic * (1.0 + gate_sum * (1.0 - logistic))
        ).astype(jnp.bfloat16)
        back[:, width + at : width + at + tile] = (back_sum * act).astype(jnp.bfloat16)
    keep = pltpu.make_async_copy(hid, hidden, hid_sem)
    keep.start()
    inv = 1.0 / total[0, 0]

    def term(left, right):
        out = lax.dot_general(
            left, right, (((0,), (0,)), ((), ())), preferred_element_type=jnp.float32
        )
        return (out * inv).astype(jnp.bfloat16)

    stores = []
    for y in range(NY):
        rows = slice(y * NX * per, (y + 1) * NX * per)
        stage[y, :, : width - cut] = term(tok[:, rows], back[:, cut:width])
        stage[y, :, width - cut :] = term(grad[:, rows], hid[...])
        stores.append(pltpu.make_async_copy(stage.at[y], by_y.at[y], out_sem.at[y]))
        stores[y].start()
    for y in range(NY):
        rows = slice(y * NX * per, (y + 1) * NX * per)
        up = term(tok[:, rows], back[:, width:])
        gate = term(tok[:, rows], back[:, :cut])
        for x in range(NX):
            by_x[x, y, :, :width] = up[x * per : (x + 1) * per]
            by_x[x, y, :, width:] = gate[x * per : (x + 1) * per]
    for store in stores:
        store.wait()
    keep.wait()


def add_x(got, out):
    acc = got[0].astype(jnp.float32)
    for i in range(1, NX):
        acc = acc + got[i].astype(jnp.float32)
    out[...] = acc.astype(jnp.bfloat16)


def turn(pos, part, *outs):
    for k, out in enumerate(outs):
        out[...] = part[(pos[1] + k) % NX]


def finish_x(*refs):
    parts, (rest, down) = refs[:NX], refs[NX:]
    acc = parts[0][...].astype(jnp.float32)
    for part in parts[1:]:
        acc = acc + part[...].astype(jnp.float32)
    cut = rest.shape[1]
    rest[...] = acc[:, :cut]
    down[...] = acc[:, cut:]


def finish(from_y, rest, gate, up):
    acc = from_y[0].astype(jnp.float32)
    for i in range(1, NY):
        acc = acc + from_y[i].astype(jnp.float32)
    width = up.shape[1]
    cut = acc.shape[1] - width
    up[...] = acc[:, :width]
    gate[:, :cut] = acc[:, width:]
    gate[:, cut:] = rest[...]


def a2a(value, axis):
    return lax.all_to_all(value, axis, split_axis=0, concat_axis=0, tiled=True)


def swap(value):
    return lax.ppermute(value, "c", [(0, 1), (1, 0)])


def along_z(value, by):
    return lax.ppermute(value, "z", [(i, (i + by) % NZ) for i in range(NZ)])


def step(
    tokens, out_grad, counts, block_moves, segment_ids, gate_weight, up_weight, down_weight
):
    bf = jnp.bfloat16
    f32 = jnp.float32
    slots, feat = tokens.shape
    per, hid = gate_weight.shape
    span = WORK * BLOCK
    model = 2 * NZ * feat
    weights = lax.all_gather(
        jnp.concatenate([gate_weight, up_weight, down_weight], axis=1), ROW, axis=0, tiled=True
    )
    pos = jnp.stack([lax.axis_index("y"), lax.axis_index("x"), counts[0], lax.axis_index("c"), lax.axis_index("z")])
    moves = block_moves.T
    box, work = pl.pallas_call(
        pack_x,
        out_shape=(
            jax.ShapeDtypeStruct((NX, 4 * BLOCK + NTAG, feat), bf),
            jax.ShapeDtypeStruct((2 * span, feat), bf),
        ),
        in_specs=[smem(), smem(), vmem(), vmem(), vmem()],
        out_specs=(vmem(), vmem()),
        scratch_shapes=[pltpu.VMEM((slots, feat), bf)],
        compiler_params=params(8),
        name="pack_x",
    )(pos, moves, segment_ids.reshape(CAP, BLOCK), tokens, out_grad)
    up2, down2 = along_z(work, 2), along_z(work, -2)
    up1, down1 = along_z(work, 1), along_z(work, -1)
    up3, down3, up4 = along_z(up2, 1), along_z(down2, -1), along_z(up2, 2)
    got = a2a(box, "x")
    box = pl.pallas_call(
        pack_y,
        out_shape=jax.ShapeDtypeStruct((NY, 2 * BLOCK + NTAG, feat), bf),
        in_specs=[smem(), smem(), vmem()],
        out_specs=vmem(),
        scratch_shapes=[pltpu.SMEM((NX,), jnp.int32)],
        compiler_params=params(8),
        name="pack_y",
    )(pos, moves, got)
    got = a2a(box, "y")
    box, total = pl.pallas_call(
        pick_arrival,
        out_shape=(
            jax.ShapeDtypeStruct((NZ, 2 * BLOCK, feat), bf),
            jax.ShapeDtypeStruct((8, BLOCK), f32),
        ),
        in_specs=[smem(), smem(), vmem()],
        out_specs=(vmem(), vmem()),
        compiler_params=params(8),
        name="pick_arrival",
    )(pos, moves, got)
    late = a2a(box, "z")
    pieces = (work, up1, up2, up3, up4, down3, down2, down1)
    mine = pl.pallas_call(
        gather_up,
        out_shape=jax.ShapeDtypeStruct((NZ, 2 * span, feat), bf),
        in_specs=[vmem()] * NZ,
        out_specs=vmem(),
        compiler_params=params(12),
        name="gather_up",
    )(*pieces)
    other = swap(mine)
    hbm = pl.BlockSpec(memory_space=pltpu.HBM)
    tok, grad = pl.pallas_call(
        lay_out,
        out_shape=(pltpu.HBM((span, model), bf), pltpu.HBM((span, model), bf)),
        in_specs=[smem(), smem(), vmem(), vmem(), vmem(), vmem()],
        out_specs=(hbm, hbm),
        scratch_shapes=[
            pltpu.VMEM((span, model), bf),
            pltpu.VMEM((span, model), bf),
            pltpu.SemaphoreType.DMA((2, NZ)),
        ],
        compiler_params=params(14),
        name="lay_out",
    )(pos, moves, mine, other, late, swap(late))

    wide_x, wide_y = hid + CUT, 2 * hid - CUT
    hidden, by_x, by_y = pl.pallas_call(
        compute,
        out_shape=(
            pltpu.HBM((span, hid), bf),
            pltpu.VMEM((NX, NY, per, wide_x), bf),
            pltpu.HBM((NY, NX * per, wide_y), bf),
        ),
        in_specs=[vmem(), hbm, hbm, hbm],
        out_specs=(hbm, vmem(), hbm),
        scratch_shapes=[
            pltpu.VMEM((span, model), bf),
            pltpu.VMEM((span, model), bf),
            pltpu.VMEM((model, 3 * hid), bf),
            pltpu.VMEM((span, hid), bf),
            pltpu.VMEM((span, 2 * hid), bf),
            pltpu.VMEM((NY, NX * per, wide_y), bf),
            pltpu.SemaphoreType.DMA((5,)),
            pltpu.SemaphoreType.DMA((NY,)),
            pltpu.SemaphoreType.DMA(()),
        ],
        compiler_params=params(36),
        name="compute",
    )(
        total,
        pltpu.with_memory_space_constraint(tok, pltpu.HBM),
        pltpu.with_memory_space_constraint(grad, pltpu.HBM),
        pltpu.with_memory_space_constraint(weights, pltpu.HBM),
    )

    part_y = lax.psum_scatter(
        by_y.reshape(NY * NX * per, wide_y), "y", scatter_dimension=0, tiled=True
    )
    part_x = pl.pallas_call(
        add_x,
        out_shape=jax.ShapeDtypeStruct((NY, per, wide_x), bf),
        in_specs=[vmem()],
        out_specs=vmem(),
        compiler_params=params(8),
        name="add_x",
    )(a2a(by_x, "x"))
    from_y = a2a(part_x, "y")
    turned = pl.pallas_call(
        turn,
        out_shape=tuple(jax.ShapeDtypeStruct((per, wide_y), bf) for _ in range(NX)),
        in_specs=[smem(), vmem()],
        out_specs=(vmem(),) * NX,
        compiler_params=params(8),
        name="turn",
    )(pos, part_y.reshape(NX, per, wide_y))
    from_x = [turned[0]] + [
        lax.ppermute(turned[k], "x", [(i, (i + k) % NX) for i in range(NX)]) for k in range(1, NX)
    ]
    rest, down_grad = pl.pallas_call(
        finish_x,
        out_shape=(
            jax.ShapeDtypeStruct((per, hid - CUT), f32),
            jax.ShapeDtypeStruct((per, hid), f32),
        ),
        in_specs=[vmem()] * NX,
        out_specs=(vmem(), vmem()),
        compiler_params=params(8),
        name="finish_x",
    )(*from_x)
    gate_grad, up_grad = pl.pallas_call(
        finish,
        out_shape=tuple(jax.ShapeDtypeStruct((per, hid), f32) for _ in range(2)),
        in_specs=[vmem(), vmem()],
        out_specs=(vmem(), vmem()),
        compiler_params=params(8),
        name="finish",
    )(from_y, rest)
    return (hidden, gate_grad, up_grad, down_grad)


def solution(mesh):
    torus = Mesh(mesh.devices.reshape(NY, NX, NZ, 2), ("y", "x", "z", "c"))
    return jax.shard_map(
        step,
        mesh=torus,
        in_specs=(P(ROW, COL), P(ROW, COL), P(ROW), P(), P(ROW), P(ROW, COL), P(ROW, COL), P(ROW, COL)),
        out_specs=(P(ROW, COL), P(ROW, COL), P(ROW, COL), P(ROW, COL)),
        check_vma=False,
    )
```
